32 devices in a mesh: grp: 2 (over x), trn: 8 (over z, y), tst: 2 (over core).
Axes of the slice: x: 2, y: 2, z: 4, core: 2. Of those that a mesh axis runs over, the one named last changes fastest.
Arguments:
- test_points: bfloat16 [64, 8192], P(None, ('grp', 'tst')), parts along dimension 1, may hold values from -9 to 9
- train_points: bfloat16 [64, 65536], P(None, ('grp', 'trn')), parts along dimension 1, may hold values from -6 to 6
- weights: bfloat16 [65536], P(('grp', 'trn')), parts along dimension 0, may hold values from -6 to 6
- factor: bfloat16 [65536, 512], P(('grp', 'trn')), parts along dimension 0, may hold values from -1.14904852 to 1.14904852
Outputs:
- mean: float32 [8192], P(('grp', 'tst')), parts along dimension 0
- variance: float32 [8192], P(('grp', 'tst')), parts along dimension 0
The draws below stay inside these ranges and needn't reach their ends.
There are 2 independent parts, one for each index of `grp`. The reference program is written for one: setup_inputs(seed, part) draws one part's arguments, and reference() takes and returns one part's arrays. A program takes and returns all parts, laid end to end along the dimension named above; each array names one. Nothing has to cross between parts.
All inputs are finite; a program needn't handle non-finite values.
Results may differ from the reference program's by a relative error of at most 0.0033.
Values sent between devices are 32-bit elements; how exact they have to be, the bound alone decides.
A program may use at most 64 MiB of HBM per device.

```python
import math
import jax
import jax.numpy as jnp
from jax import lax

DIM = 64
RANK = 512
TEST = 4096
TRAIN = 32768


def points_of(key):
    base_key = jax.random.fold_in(key, 11)
    train = jnp.clip(jax.random.normal(base_key, (DIM, TRAIN), jnp.float32), -6.0, 6.0)
    return train


def draw_train_points(key, part):
    return points_of(key).astype(jnp.bfloat16)


def draw_test_points(key, part):
    train = points_of(key)
    anchor = jax.random.randint(jax.random.fold_in(key, 12), (TEST,), 0, TRAIN)
    noise = jnp.clip(jax.random.normal(jax.random.fold_in(key, 13), (DIM, TEST), jnp.float32), -6.0, 6.0)
    spread = jnp.full((1, TEST), 0.5, jnp.float32)
    return (jnp.take(train, anchor, axis=1) + spread * noise).astype(jnp.bfloat16)


def draw_factor(key, part):
    base = jnp.clip(jax.random.normal(jax.random.fold_in(key, 21), (TRAIN, RANK), jnp.float32), -6.0, 6.0)
    return (base * (0.9 / math.sqrt(RANK))).astype(jnp.bfloat16)


def shard_levels(own_key, dims, pieces, low, high):
    def one(position, parts):
        steps = jax.random.uniform(jax.random.fold_in(jax.random.fold_in(own_key, 6), position), (parts,), jnp.float32, low / len(pieces), high / len(pieces))
        return jnp.repeat(jnp.exp(steps), dims[position] // parts).reshape((-1,) + (1,) * (len(dims) - position - 1))

    level = one(*pieces[0])
    for cut in pieces[1:]:
        level = level * one(*cut)
    return level


def normal_values(key, shape, scale, reach, split=(), kind=jnp.bfloat16):
    entries = jax.random.normal(key, shape, jnp.float32) * scale
    if len(split) > 0:
        entries = shard_levels(key, shape, split, -0.22, 0.18) * entries
    return jnp.clip(entries, min=-reach, max=reach).astype(kind)


def setup_inputs(seed: int = 0, part: int = 0) -> dict:
    streams_of = jax.random.split(jax.random.key(seed), 5)
    part_keys = jax.random.split(jax.random.fold_in(streams_of[4], part), 5)
    test_points = draw_test_points(jax.random.fold_in(jax.random.fold_in(streams_of[4], part), 71), part)
    train_points = draw_train_points(jax.random.fold_in(jax.random.fold_in(streams_of[4], part), 71), part)
    weights = normal_values(part_keys[2], (TRAIN,), 1.5, 6.0, ((0, 8),))
    factor = draw_factor(jax.random.fold_in(jax.random.fold_in(streams_of[4], part), 71), part)
    return dict(test_points=test_points, train_points=train_points, weights=weights, factor=factor)


def reference(test_points, train_points, weights, factor):
    test_sq = jnp.sum(test_points.astype(jnp.float32) ** 2, axis=0)
    total = train_points.shape[1]
    block = math.gcd(total, 1024)
    count = total // block
    width = factor.shape[1]
    rows = test_points.shape[1]

    def step(carry, index):
        mean_acc, proj_acc = carry
        start = (index * block).astype(jnp.int32)
        points = lax.dynamic_slice_in_dim(train_points, start, block, 1)
        wblock = lax.dynamic_slice_in_dim(weights, start, block, 0)
        fblock = lax.dynamic_slice_in_dim(factor, start, block, 0)
        train_sq = jnp.sum(points.astype(jnp.float32) ** 2, axis=0)
        cross = jnp.dot(test_points.T, points, preferred_element_type=jnp.float32)
        kernel = jnp.exp(-(test_sq[:, None] + train_sq[None, :] - 2.0 * cross) * (4.0 / DIM)).astype(jnp.bfloat16)
        mean_acc = mean_acc + jnp.dot(kernel, wblock, preferred_element_type=jnp.float32)
        proj_acc = proj_acc + jnp.dot(kernel, fblock, preferred_element_type=jnp.float32)
        return (mean_acc, proj_acc), None

    init = (jnp.zeros((rows,), jnp.float32), jnp.zeros((rows, width), jnp.float32))
    (mean, project), _ = lax.scan(step, init, jnp.arange(count, dtype=jnp.int32))
    variance = 1.0 - jnp.sum(project * project, axis=1)
    return mean, variance
```

```python
import functools
import math

import jax
import jax.numpy as jnp
from jax import lax
from jax.experimental import pallas as pl
from jax.experimental.pallas import tpu as pltpu
from jax.sharding import PartitionSpec as P

LOG2E = 1.4426950408889634
BLOCK = 128
CHUNK = 1024
LINE = 4
KINDS = ((8, 16, 16), (8, 8, 24))
LAG_Y = 3
LAG_B = (0, 2, 4, 11)
LAG_A = (3, 5, 8, 25)
LAG_SWAP = 13
LAG_X = 23
MEAN_AT = 1
MEAN_ON = 4


def pieces(value):
    high = value.astype(jnp.bfloat16).astype(jnp.float32)
    rest = value - high
    middle = rest.astype(jnp.bfloat16).astype(jnp.float32)
    low = (rest - middle).astype(jnp.bfloat16).astype(jnp.float32)
    return high, middle, low


def pick(row, table, default):
    value = default
    for index, entry in table:
        value = jnp.where(row == index, entry, value)
    return value


def kinds_of(rows):
    unit = rows // BLOCK // sum(count for count, _, _ in KINDS)
    table, begin, base = [], 0, 0
    for count, gb, ga in KINDS:
        count = count * unit
        table.append((begin, count, gb, ga, base))
        begin += count
        base += count * (gb + ga)
    return tuple(table)


def kernel(
    test_hbm, train_hbm, weights_hbm, factor_hbm, out_ref,
    test_ref, train_ref, weights_ref, factor_ref, in_sems,
    test_aug, train_aug, wide, left_ref, part, mean_acc, var_acc, mean_box, var_box,
    s_y, r_y, s_br, r_br, s_bl, r_bl, s_ar, r_ar, s_al, r_al, s_x, r_x,
    s_mean, r_mean, s_var, r_var, *got,
):
    count = var_box.shape[0] * 2
    pair = count // LINE
    last = LINE - 1
    me = lax.axis_index("trn")
    z = me // pair
    y = me % pair
    dim, rows = test_ref.shape
    local = train_ref.shape[1]
    depth = test_aug.shape[1]
    steps = rows // BLOCK
    kinds = kinds_of(rows)
    span = rows // 4
    other = z * pair + (1 - y)
    up, down = me + pair, me - pair
    chunks = local // CHUNK

    barrier = pltpu.get_barrier_semaphore()
    for k in range(1, count):
        pl.semaphore_signal(barrier, inc=1, device_id={"trn": lax.rem(me + k, count)})

    def fetch(index, source, target):
        return pltpu.make_async_copy(source, target, in_sems.at[index])

    fetch_train = fetch(0, train_hbm, train_ref)
    fetch_test = fetch(1, test_hbm, test_ref)
    fetch_weights = fetch(2, weights_hbm, weights_ref)

    def fetch_factor(index):
        block = pl.ds(index * CHUNK, CHUNK)
        return fetch(3 + index, factor_hbm.at[block], factor_ref.at[block])

    fetch_train.start()
    fetch_test.start()
    fetch_weights.start()
    for index in range(chunks):
        fetch_factor(index).start()

    fetch_train.wait()

    def prepare_train(index, carry):
        cols = pl.ds(pl.multiple_of(index * 512, 512), 512)
        points = train_ref[:, cols]
        squares = points.astype(jnp.float32) ** 2
        norm = jnp.sum(squares, axis=0, keepdims=True) * (-4.0 / dim)
        high, middle, low = pieces(norm)
        row = lax.broadcasted_iota(jnp.int32, (16, 512), 0)
        one = jnp.float32(1.0)
        extra = pick(row, ((0, one), (1, one), (2, one), (3, high), (4, middle), (5, low)), jnp.float32(0.0))
        train_aug[:dim, cols] = points
        train_aug[dim : dim + 16, cols] = extra.astype(jnp.bfloat16)
        train_aug[dim + 16 :, cols] = jnp.zeros((depth - dim - 16, 512), jnp.bfloat16)
        return carry

    lax.fori_loop(0, local // 512, prepare_train, 0)
    fetch_test.wait()

    def prepare_test(index, carry):
        cols = pl.ds(pl.multiple_of(index * 256, 256), 256)
        points = test_ref[:, cols].astype(jnp.float32)
        norm = jnp.sum(points * points, axis=0, keepdims=True) * (-4.0 / dim)
        high, middle, low = pieces(norm)
        row = lax.broadcasted_iota(jnp.int32, (8, 256), 0)
        one = jnp.float32(1.0)
        extra = pick(row, ((0, high), (1, middle), (2, low), (3, one), (4, one), (5, one)), jnp.float32(0.0))
        whole = jnp.concatenate(
            [points * (8.0 / dim), extra, jnp.zeros((depth - dim - 8, 256), jnp.float32)], axis=0
        )
        test_aug[cols, :] = whole.T
        return carry

    lax.fori_loop(0, rows // 256, prepare_test, 0)
    fetch_weights.wait()
    for index in range(local // 128):
        wide[:, index * 128 : (index + 1) * 128] = weights_ref[index : index + 1, :].astype(jnp.float32)

    def places(kind, step):
        begin, number, gb, ga, base = kind
        index = step - begin

        def row_of(owner, early):
            inner = base + (number * gb + index * ga if early else index * gb)
            return pl.multiple_of(owner * span + inner, 8)

        where = (
            row_of(2, False), row_of(3, False), row_of(0, False), row_of(1, False),
            row_of(1 - y, True), row_of(3 - y, True), row_of(y, True), row_of(2 + y, True),
        )
        return tuple(zip(where, (gb,) * 4 + (ga,) * 4))

    def compute(step, first=False):
        for kind in kinds:
            if first and kind[0] > 0:
                continue

            def gather():
                left_ref[...] = jnp.concatenate(
                    [test_aug[pl.ds(at, size), :] for at, size in places(kind, step)], axis=0
                ).astype(jnp.bfloat16)

            if first:
                gather()
            else:
                pl.when((step >= kind[0]) & (step < kind[0] + kind[1]))(gather)
        left = left_ref[...]
        total = None
        means = None
        for index in range(chunks):
            begin = index * CHUNK
            power = jnp.dot(
                left, train_aug[:, begin : begin + CHUNK], preferred_element_type=jnp.float32
            )
            values = jnp.exp2(power * LOG2E).astype(jnp.bfloat16)
            scaled = values.astype(jnp.float32) * wide[:, begin : begin + CHUNK]
            for lane in range(0, CHUNK, 128):
                piece = scaled[:, lane : lane + 128]
                means = piece if means is None else means + piece
            if first:
                fetch_factor(index).wait()
            product = jnp.dot(
                values, factor_ref[begin : begin + CHUNK, :], preferred_element_type=jnp.float32
            )
            total = product if total is None else total + product
        part[step] = total
        mean_acc[pl.ds(pl.multiple_of(step * BLOCK, BLOCK), BLOCK), :] = means

    def send(source, target, ssem, rsem, device):
        return pltpu.make_async_remote_copy(
            src_ref=source, dst_ref=target, send_sem=ssem, recv_sem=rsem, device_id={"trn": device}
        )

    def square(values):
        total = None
        for lane in range(0, values.shape[1], 128):
            piece = values[:, lane : lane + 128]
            total = piece * piece if total is None else total + piece * piece
        return total

    class Kind:
        def __init__(self, kind, buffers):
            self.begin, self.number, self.gb, self.ga, self.base = kind
            self.got_y, self.got_br, self.got_bl, self.got_ar, self.got_al, self.got_x = buffers
            gb, ga = self.gb, self.ga
            self.chains_b = (
                (self.got_br, 0, s_br, r_br, z, up),
                (self.got_bl, 2 * gb, s_bl, r_bl, last - z, down),
            )
            self.chains_a = (
                (self.got_ar, 4 * gb + 3 * ga, s_ar, r_ar, z, up),
                (self.got_al, 4 * gb + 2 * ga, s_al, r_al, last - z, down),
            )

        def has(self, s):
            return (s >= self.begin) & (s < self.begin + self.number)

        def copy_y(self, s):
            gb, ga = self.gb, self.ga
            source = part.at[s, 4 * gb : 4 * gb + 2 * ga]
            return send(source, self.got_y.at[s - self.begin], s_y.at[s], r_y.at[s], other)

        def first_b(self, s, chain):
            got, begin, ssem, rsem, _, device = chain
            source = part.at[s, begin : begin + 2 * self.gb]
            return send(source, got.at[s - self.begin], ssem.at[s], rsem.at[s], device)

        def first_a(self, s, chain):
            got, begin, ssem, rsem, _, device = chain
            source = part.at[s, begin : begin + self.ga]
            return send(source, got.at[s - self.begin], ssem.at[s], rsem.at[s], device)

        def onward(self, s, chain):
            got, _, ssem, rsem, _, device = chain
            j = s - self.begin
            return send(got.at[j], got.at[j], ssem.at[s], rsem.at[s], device)

        def swap(self, s, got):
            j = s - self.begin
            theirs = pl.ds(pl.multiple_of((1 - y) * self.gb, 8), self.gb)
            return send(got.at[j, theirs], self.got_x.at[j], s_x.at[s], r_x.at[s], other)

    table = [Kind(kind, got[6 * i : 6 * i + 6]) for i, kind in enumerate(kinds)]

    def lag_of(hop, lags):
        value = lags[1]
        for index in range(2, LINE):
            value = jnp.where(hop == index, lags[index], value)
        return value

    def mean_swap():
        return send(mean_box.at[z], mean_box.at[LINE], s_mean.at[0], r_mean.at[0], other)

    def mean_copy(k):
        target = lax.rem(me + k * pair, count)
        return send(mean_box.at[z], mean_box.at[z], s_mean.at[k], r_mean.at[k], target)

    compute(0, True)
    pl.semaphore_wait(barrier, count - 1)

    def turn(it, carry):
        @pl.when((it > 0) & (it < steps))
        def _():
            compute(it)

        for kind in table:
            @pl.when(kind.has(it))
            def _():
                for chain in kind.chains_b:
                    @pl.when(chain[4] == 0)
                    def _():
                        kind.first_b(it, chain).start()
                kind.copy_y(it).start()

        for kind in table:
            gb = kind.gb
            for chain in kind.chains_b:
                got, begin, hop = chain[0], chain[1], chain[4]
                s = it - lag_of(hop, LAG_B)

                @pl.when((hop > 0) & kind.has(s))
                def _():
                    kind.onward(s, chain).wait_recv()
                    j = s - kind.begin
                    got[j] = got[j] + part[s, begin : begin + 2 * gb]

                    @pl.when(hop < last)
                    def _():
                        kind.onward(s, chain).start()

        for kind in table:
            gb, ga = kind.gb, kind.ga
            s_here = it - LAG_Y

            @pl.when(kind.has(s_here))
            def _():
                kind.copy_y(s_here).wait_recv()
                kept = slice(4 * gb + 2 * ga, 4 * gb + 4 * ga)
                part[s_here, kept] = part[s_here, kept] + kind.got_y[s_here - kind.begin]

            s_go = it - LAG_A[0]

            @pl.when(kind.has(s_go))
            def _():
                for chain in kind.chains_a:
                    @pl.when(chain[4] == 0)
                    def _():
                        kind.first_a(s_go, chain).start()

        for kind in table:
            gb, ga = kind.gb, kind.ga
            for chain in kind.chains_a:
                got, begin, hop = chain[0], chain[1], chain[4]
                s = it - lag_of(hop, LAG_A)

                @pl.when((hop > 0) & kind.has(s))
                def _():
                    kind.onward(s, chain).wait_recv()
                    j = s - kind.begin

                    @pl.when(hop < last)
                    def _():
                        got[j] = got[j] + part[s, begin : begin + ga]
                        kind.onward(s, chain).start()

                    @pl.when(hop == last)
                    def _():
                        at = pl.multiple_of(kind.base + gb * kind.number + j * ga, 8)
                        var_acc[pl.ds(at, ga), :] = square(got[j] + part[s, begin : begin + ga])

        for kind in table:
            gb = kind.gb
            s_swap = it - LAG_SWAP
            s_last = it - LAG_X
            for got, hop in ((kind.got_br, z), (kind.got_bl, last - z)):
                @pl.when((hop == last) & kind.has(s_swap))
                def _():
                    kind.swap(s_swap, got).start()

                @pl.when((hop == last) & kind.has(s_last))
                def _():
                    kind.swap(s_last, got).wait_recv()
                    j = s_last - kind.begin
                    mine = pl.ds(pl.multiple_of(y * gb, 8), gb)
                    at = pl.multiple_of(kind.base + j * gb, 8)
                    var_acc[pl.ds(at, gb), :] = square(got[j, mine] + kind.got_x[j])

        @pl.when(it == steps + MEAN_AT)
        def _():
            for kind in kinds:
                def place(step, carry):
                    begin = pl.multiple_of(step * BLOCK, BLOCK)
                    for at, size in places(kind, step):
                        test_aug[pl.ds(at, size), :] = mean_acc[pl.ds(begin, size), :]
                        begin = pl.multiple_of(begin + size, 8)
                    return carry

                lax.fori_loop(kind[0], kind[0] + kind[1], place, 0)
            for index in range(rows // 128):
                block = test_aug[index * 128 : (index + 1) * 128, :]
                mean_box[z, index : index + 1, :] = jnp.sum(block.T, axis=0, keepdims=True)
            mean_swap().start()

        @pl.when(it == steps + MEAN_ON)
        def _():
            mean_swap().wait()
            mean_box[z] = mean_box[z] + mean_box[LINE]
            for k in range(1, LINE):
                mean_copy(k).start()

        return carry

    lax.fori_loop(0, steps + max(LAG_X, LAG_A[-1]), turn, 0)

    owner = jnp.where(z == last, 2, 0) + y
    ends = (z == 0) | (z == last)

    def var_copy(k, who):
        return send(var_box.at[who], var_box.at[who], s_var.at[k], r_var.at[who], lax.rem(me + k, count))

    @pl.when(ends)
    def _():
        for index in range(span // 128):
            block = var_acc[index * 128 : (index + 1) * 128, :]
            var_box[owner, index : index + 1, :] = 1.0 - jnp.sum(block.T, axis=0, keepdims=True)
        for k in range(1, count):
            var_copy(k, owner).start()

    for k in range(1, LINE):
        mean_copy(k).wait()
    total = mean_box[0]
    for index in range(1, LINE):
        total = total + mean_box[index]
    out_ref[: rows // 128, :] = total

    for kind in table:
        def settle(s, carry):
            kind.copy_y(s).wait_send()
            for chain in kind.chains_b:
                got, hop = chain[0], chain[4]

                @pl.when(hop == 0)
                def _():
                    kind.first_b(s, chain).wait_send()

                @pl.when((hop > 0) & (hop < last))
                def _():
                    kind.onward(s, chain).wait_send()

                @pl.when(hop == last)
                def _():
                    kind.swap(s, got).wait_send()

            for chain in kind.chains_a:
                hop = chain[4]

                @pl.when(hop == 0)
                def _():
                    kind.first_a(s, chain).wait_send()

                @pl.when((hop > 0) & (hop < last))
                def _():
                    kind.onward(s, chain).wait_send()

            return carry

        lax.fori_loop(kind.begin, kind.begin + kind.number, settle, 0)

    for who in range(4):
        @pl.when(jnp.logical_not(ends) | (owner != who))
        def _():
            var_copy(1, who).wait_recv()

    lines = span // 128
    for who in range(4):
        begin = rows // 128 + who * lines
        out_ref[begin : begin + lines, :] = var_box[who]

    @pl.when(ends)
    def _():
        for k in range(1, count):
            var_copy(k, owner).wait_send()


def fused(test_points, train_points, weights, factor, *, count):
    dim, rows = test_points.shape
    local = train_points.shape[1]
    width = factor.shape[1]
    depth = -(-(dim + 16) // 128) * 128
    steps = rows // BLOCK
    dma = pltpu.SemaphoreType.DMA
    f32 = jnp.float32
    sems = [dma((steps,))] * 12 + [dma((LINE,)), dma((LINE,)), dma((count,)), dma((4,))]
    boxes = []
    for _, number, gb, ga, _ in kinds_of(rows):
        for size in (2 * ga, 2 * gb, 2 * gb, ga, ga, gb):
            boxes.append(pltpu.VMEM((number, size, width), f32))
    out = pl.pallas_call(
        kernel,
        out_shape=jax.ShapeDtypeStruct((rows // 64, 128), f32),
        in_specs=[pl.BlockSpec(memory_space=pl.ANY)] * 4,
        out_specs=pl.BlockSpec(memory_space=pltpu.VMEM),
        scratch_shapes=[
            pltpu.VMEM((dim, rows), jnp.bfloat16),
            pltpu.VMEM((dim, local), jnp.bfloat16),
            pltpu.VMEM((local // 128, 128), jnp.bfloat16),
            pltpu.VMEM((local, width), jnp.bfloat16),
            dma((3 + local // CHUNK,)),
            pltpu.VMEM((rows, depth), f32),
            pltpu.VMEM((depth, local), jnp.bfloat16),
            pltpu.VMEM((1, local), f32),
            pltpu.VMEM((BLOCK, depth), jnp.bfloat16),
            pltpu.VMEM((steps, BLOCK, width), f32),
            pltpu.VMEM((rows, 128), f32),
            pltpu.VMEM((rows // 4, 128), f32),
            pltpu.VMEM((LINE + 1, rows // 128, 128), f32),
            pltpu.VMEM((4, rows // 512, 128), f32),
        ] + sems + boxes,
        compiler_params=pltpu.CompilerParams(
            collective_id=0, has_side_effects=True, vmem_limit_bytes=56 * 1024 * 1024
        ),
    )(test_points, train_points, weights.reshape(local // 128, 128), factor)
    lines = rows // 128
    return out[:lines].reshape(rows), out[lines:].reshape(rows)


def on_device(test_points, train_points, weights, factor):
    rows = test_points.shape[1]
    local = train_points.shape[1]
    dim = test_points.shape[0]
    width = factor.shape[1]
    test_sq = jnp.sum(test_points.astype(jnp.float32) ** 2, axis=0)
    block = math.gcd(local, 1024)
    turns = local // block

    def step(index, carry):
        mean_acc, proj_acc = carry
        start = (index * block).astype(jnp.int32)
        points = lax.dynamic_slice_in_dim(train_points, start, block, 1)
        wblock = lax.dynamic_slice_in_dim(weights, start, block, 0)
        fblock = lax.dynamic_slice_in_dim(factor, start, block, 0)
        train_sq = jnp.sum(points.astype(jnp.float32) ** 2, axis=0)
        cross = lax.dot_general(
            test_points, points, (((0,), (0,)), ((), ())), preferred_element_type=jnp.float32
        )
        kernel = jnp.exp(
            -(test_sq[:, None] + train_sq[None, :] - 2.0 * cross) * (4.0 / dim)
        ).astype(jnp.bfloat16)
        mean_acc = mean_acc + jnp.dot(kernel, wblock, preferred_element_type=jnp.float32)
        proj_acc = proj_acc + jnp.dot(kernel, fblock, preferred_element_type=jnp.float32)
        return (mean_acc, proj_acc)

    init = (jnp.zeros((rows,), jnp.float32), jnp.zeros((rows, width), jnp.float32))
    mean_part, proj_part = lax.fori_loop(0, turns, step, init)
    mean_share, proj_share = (
        lax.psum_scatter(mean_part, "trn", scatter_dimension=0, tiled=True),
        lax.psum_scatter(proj_part, "trn", scatter_dimension=0, tiled=True),
    )
    var_share = 1.0 - jnp.sum(proj_share * proj_share, axis=1)
    mean, variance = (
        lax.all_gather(mean_share, "trn", axis=0, tiled=True),
        lax.all_gather(var_share, "trn", axis=0, tiled=True),
    )
    return (mean, variance)


def solution(mesh):
    in_specs = (
        P(None, ("grp", "tst")),
        P(None, ("grp", "trn")),
        P(("grp", "trn")),
        P(("grp", "trn"), None),
    )
    out_specs = (P(("grp", "tst")), P(("grp", "tst")))
    count = mesh.shape["trn"]
    body = functools.partial(fused, count=count) if count == 2 * LINE else on_device
    return jax.shard_map(
        body, mesh=mesh, in_specs=in_specs, out_specs=out_specs, check_vma=False
    )
```

```python
import functools
import math

import jax
import jax.numpy as jnp
from jax import lax
from jax.experimental import pallas as pl
from jax.experimental.pallas import tpu as pltpu
from jax.sharding import PartitionSpec as P

LOG2E = 1.4426950408889634
BLOCK = 128
CHUNK = 1024
LINE = 4
KINDS = ((10, 16, 16), (4, 8, 24))
MIDDLE = 2
LAG_Y = 3
LAG_B = (0, 2, 4, 11)
LAG_A = (3, 5, 8, 18)
LAG_SWAP = 11
LAG_X = 18
LAG_M = (4, 6, 17)
MEAN_AT = 1
MEAN_ON = 4


def pieces(value):
    high = value.astype(jnp.bfloat16).astype(jnp.float32)
    rest = value - high
    middle = rest.astype(jnp.bfloat16).astype(jnp.float32)
    low = (rest - middle).astype(jnp.bfloat16).astype(jnp.float32)
    return high, middle, low


def pick(row, table, default):
    value = default
    for index, entry in table:
        value = jnp.where(row == index, entry, value)
    return value


def kinds_of(rows):
    unit = rows // BLOCK // (MIDDLE + sum(count for count, _, _ in KINDS))
    table, begin, base = [], 0, 0
    for count, gb, ga in KINDS:
        count = count * unit
        table.append((begin, count, gb, ga, base))
        begin += count
        base += count * (gb + ga)
    return tuple(table), (begin, MIDDLE * unit, BLOCK // 4, base)


def kernel(
    test_hbm, train_hbm, weights_hbm, factor_hbm, out_ref,
    test_ref, train_ref, weights_ref, factor_ref, in_sems,
    test_aug, train_aug, wide, left_ref, part, mean_acc, var_acc, mean_box, var_box, mid_box,
    s_y, r_y, s_b, rp_b, sq_b, rq_b, s_a, rp_a, sq_a, rq_a, s_x, r_x,
    s_yn, r_yn, s_mf, r_mf, s_mn, r_mn, s_mx, r_mx,
    s_mean, r_mean, s_var, r_var, r_mid, got_yf, got_yn, got_mf, got_mn, got_mx, *got, count,
):
    pair = count // LINE
    last = LINE - 1
    me = lax.axis_index("trn")
    z = me // pair
    y = me % pair
    dim, rows = test_ref.shape
    local = train_ref.shape[1]
    depth = test_aug.shape[1]
    steps = rows // BLOCK
    kinds, middle = kinds_of(rows)
    span = rows // 4
    other = z * pair + (1 - y)
    low = z < 2
    toward = jnp.where(low, me + pair, me - pair)
    back = jnp.where(low, me - pair, me + pair)
    far = jnp.where(low, 2, 0)
    near = 2 - far
    owner = near + y
    ends = (z == 0) | (z == last)
    chunks = local // CHUNK

    barrier = pltpu.get_barrier_semaphore()
    for k in range(1, count):
        pl.semaphore_signal(barrier, inc=1, device_id={"trn": lax.rem(me + k, count)})

    def fetch(index, source, target):
        return pltpu.make_async_copy(source, target, in_sems.at[index])

    fetch_train = fetch(0, train_hbm, train_ref)
    fetch_test = fetch(1, test_hbm, test_ref)
    fetch_weights = fetch(2, weights_hbm, weights_ref)

    def fetch_factor(index):
        block = pl.ds(index * CHUNK, CHUNK)
        return fetch(3 + index, factor_hbm.at[block], factor_ref.at[block])

    fetch_train.start()
    fetch_test.start()
    fetch_weights.start()
    for index in range(chunks):
        fetch_factor(index).start()

    var_acc[...] = jnp.zeros_like(var_acc)
    fetch_train.wait()

    def prepare_train(index, carry):
        cols = pl.ds(pl.multiple_of(index * 512, 512), 512)
        points = train_ref[:, cols]
        squares = points.astype(jnp.float32) ** 2
        norm = jnp.sum(squares, axis=0, keepdims=True) * (-4.0 / dim)
        high, middle, low = pieces(norm)
        row = lax.broadcasted_iota(jnp.int32, (16, 512), 0)
        one = jnp.float32(1.0)
        extra = pick(row, ((0, one), (1, one), (2, one), (3, high), (4, middle), (5, low)), jnp.float32(0.0))
        train_aug[:dim, cols] = points
        train_aug[dim : dim + 16, cols] = extra.astype(jnp.bfloat16)
        train_aug[dim + 16 :, cols] = jnp.zeros((depth - dim - 16, 512), jnp.bfloat16)
        return carry

    lax.fori_loop(0, local // 512, prepare_train, 0)
    fetch_test.wait()

    def prepare_test(index, carry):
        cols = pl.ds(pl.multiple_of(index * 256, 256), 256)
        points = test_ref[:, cols].astype(jnp.float32)
        norm = jnp.sum(points * points, axis=0, keepdims=True) * (-4.0 / dim)
        high, middle, low = pieces(norm)
        row = lax.broadcasted_iota(jnp.int32, (8, 256), 0)
        one = jnp.float32(1.0)
        extra = pick(row, ((0, high), (1, middle), (2, low), (3, one), (4, one), (5, one)), jnp.float32(0.0))
        whole = jnp.concatenate(
            [points * (8.0 / dim), extra, jnp.zeros((depth - dim - 8, 256), jnp.float32)], axis=0
        )
        test_aug[cols, :] = whole.T
        return carry

    lax.fori_loop(0, rows // 256, prepare_test, 0)
    fetch_weights.wait()
    for index in range(local // 128):
        wide[:, index * 128 : (index + 1) * 128] = weights_ref[index : index + 1, :].astype(jnp.float32)

    def edge_places(kind, step):
        begin, number, gb, ga, base = kind
        index = step - begin

        def row_of(who, early):
            inner = base + (number * gb + index * ga if early else index * gb)
            return pl.multiple_of(who * span + inner, 8)

        where = (
            row_of(far, False), row_of(far + 1, False), row_of(near, False), row_of(near + 1, False),
            row_of(far + 1 - y, True), row_of(near + 1 - y, True), row_of(far + y, True), row_of(near + y, True),
        )
        return tuple(zip(where, (gb,) * 4 + (ga,) * 4))

    def middle_places(step):
        begin, _, gm, base = middle
        inner = base + (step - begin) * gm
        who = (far + 1 - y, near + 1 - y, far + y, near + y)
        return tuple((pl.multiple_of(w * span + inner, 8), gm) for w in who)

    layouts = [(kind[0], kind[1], functools.partial(edge_places, kind)) for kind in kinds]
    layouts.append((middle[0], middle[1], middle_places))

    def compute(step, first=False):
        for begin, number, places in layouts:
            if first and begin > 0:
                continue

            def gather():
                left_ref[...] = jnp.concatenate(
                    [test_aug[pl.ds(at, size), :] for at, size in places(step)], axis=0
                ).astype(jnp.bfloat16)

            if first:
                gather()
            else:
                pl.when((step >= begin) & (step < begin + number))(gather)
        left = left_ref[...]
        total = None
        means = None
        for index in range(chunks):
            begin = index * CHUNK
            power = jnp.dot(
                left, train_aug[:, begin : begin + CHUNK], preferred_element_type=jnp.float32
            )
            values = jnp.exp2(power * LOG2E).astype(jnp.bfloat16)
            scaled = values.astype(jnp.float32) * wide[:, begin : begin + CHUNK]
            for lane in range(0, CHUNK, 128):
                piece = scaled[:, lane : lane + 128]
                means = piece if means is None else means + piece
            if first:
                fetch_factor(index).wait()
            product = jnp.dot(
                values, factor_ref[begin : begin + CHUNK, :], preferred_element_type=jnp.float32
            )
            total = product if total is None else total + product
        part[step] = total
        mean_acc[pl.ds(pl.multiple_of(step * BLOCK, BLOCK), BLOCK), :] = means

    def send(source, target, ssem, rsem, device):
        return pltpu.make_async_remote_copy(
            src_ref=source, dst_ref=target, send_sem=ssem, recv_sem=rsem, device_id={"trn": device}
        )

    def square(values):
        total = None
        for lane in range(0, values.shape[1], 128):
            piece = values[:, lane : lane + 128]
            total = piece * piece if total is None else total + piece * piece
        return total

    class Kind:
        def __init__(self, kind, buffers):
            self.begin, self.number, self.gb, self.ga, self.base = kind
            self.got_y, self.bp, self.bq, self.ap, self.aq, self.got_x = buffers
            gb, ga = self.gb, self.ga
            self.sent = slice(4 * gb, 4 * gb + 2 * ga)
            self.kept = slice(4 * gb + 2 * ga, 4 * gb + 4 * ga)
            self.out_b, self.in_b = slice(0, 2 * gb), slice(2 * gb, 4 * gb)
            self.out_a = slice(4 * gb + 2 * ga, 4 * gb + 3 * ga)
            self.in_a = slice(4 * gb + 3 * ga, 4 * gb + 4 * ga)

        def has(self, s):
            return (s >= self.begin) & (s < self.begin + self.number)

        def copy_y(self, s):
            return send(part.at[s, self.sent], self.got_y.at[s - self.begin], s_y.at[s], r_y.at[s], other)

        def first_b(self, s):
            return send(part.at[s, self.out_b], self.bp.at[s - self.begin], s_b.at[s], rp_b.at[s], toward)

        def cross_b(self, s):
            j = s - self.begin
            return send(self.bp.at[j], self.bq.at[j], s_b.at[s], rq_b.at[s], toward)

        def back_b(self, s):
            j = s - self.begin
            return send(self.bq.at[j], self.bq.at[j], sq_b.at[s], rq_b.at[s], back)

        def first_a(self, s):
            return send(part.at[s, self.out_a], self.ap.at[s - self.begin], s_a.at[s], rp_a.at[s], toward)

        def cross_a(self, s):
            j = s - self.begin
            return send(self.ap.at[j], self.aq.at[j], s_a.at[s], rq_a.at[s], toward)

        def back_a(self, s):
            j = s - self.begin
            return send(self.aq.at[j], self.aq.at[j], sq_a.at[s], rq_a.at[s], back)

        def swap(self, s):
            j = s - self.begin
            theirs = pl.ds(pl.multiple_of((1 - y) * self.gb, 8), self.gb)
            return send(self.bq.at[j, theirs], self.got_x.at[j], s_x.at[s], r_x.at[s], other)

    table = [Kind(kind, got[6 * i : 6 * i + 6]) for i, kind in enumerate(kinds)]
    m_begin, m_number, gm, m_base = middle

    def m_has(s):
        return (s >= m_begin) & (s < m_begin + m_number)

    def m_y(s):
        j = s - m_begin
        return (
            send(part.at[s, :gm], got_yf.at[j], s_y.at[s], r_y.at[s], other),
            send(part.at[s, gm : 2 * gm], got_yn.at[j], s_yn.at[j], r_yn.at[j], other),
        )

    def m_first(s):
        j = s - m_begin
        return (
            send(part.at[s, 2 * gm : 3 * gm], got_mf.at[j], s_mf.at[j], r_mf.at[j], toward),
            send(part.at[s, 3 * gm :], got_mn.at[j], s_mn.at[j], r_mn.at[j], toward),
        )

    def m_cross(s):
        j = s - m_begin
        return send(got_mf.at[j], got_mx.at[j], s_mx.at[j], r_mx.at[j], toward)

    def mean_swap():
        return send(mean_box.at[z], mean_box.at[LINE], s_mean.at[0], r_mean.at[0], other)

    def mean_copy(k):
        target = lax.rem(me + k * pair, count)
        return send(mean_box.at[z], mean_box.at[z], s_mean.at[k], r_mean.at[k], target)

    def mean_start():
        for begin, number, places in layouts:
            def place(step, carry):
                start = pl.multiple_of(step * BLOCK, BLOCK)
                for at, size in places(step):
                    test_aug[pl.ds(at, size), :] = mean_acc[pl.ds(start, size), :]
                    start = pl.multiple_of(start + size, 8)
                return carry

            lax.fori_loop(begin, begin + number, place, 0)
        for index in range(rows // 128):
            block = test_aug[index * 128 : (index + 1) * 128, :]
            mean_box[z, index : index + 1, :] = jnp.sum(block.T, axis=0, keepdims=True)
        mean_swap().start()

    def mean_spread():
        mean_swap().wait()
        mean_box[z] = mean_box[z] + mean_box[LINE]
        for k in range(1, LINE):
            mean_copy(k).start()

    lines = span // 128

    def line_of(index):
        block = var_acc[index * 128 : (index + 1) * 128, :]
        return jnp.sum(block.T, axis=0, keepdims=True)

    def var_copy(k, who):
        return send(var_box.at[who], var_box.at[who], s_var.at[k], r_var.at[who], lax.rem(me + k, count))

    def mid_copy(k, who):
        return send(mid_box.at[who], mid_box.at[who], s_var.at[k], r_mid.at[who], lax.rem(me + k, count))

    def receive_y(it):
        for kind in table:
            s = it - LAG_Y

            @pl.when(kind.has(s))
            def _():
                kind.copy_y(s).wait_recv()
                part[s, kind.kept] = part[s, kind.kept] + kind.got_y[s - kind.begin]

    def receive_m(s):
        j = s - m_begin
        yf, yn = m_y(s)
        yf.wait_recv()
        part[s, 2 * gm : 3 * gm] = part[s, 2 * gm : 3 * gm] + got_yf[j]
        yield
        yn.wait_recv()
        part[s, 3 * gm :] = part[s, 3 * gm :] + got_yn[j]

    def send_y(it):
        for kind in table:
            pl.when(kind.has(it))(lambda: kind.copy_y(it).start())

        @pl.when(m_has(it))
        def _():
            for copy in m_y(it):
                copy.start()

    def means(it):
        pl.when(it == steps + MEAN_AT)(mean_start)
        pl.when(it == steps + MEAN_ON)(mean_spread)

    def end_turn(it, carry):
        pl.when((it > 0) & (it < steps))(lambda: compute(it))
        for kind in table:
            pl.when(kind.has(it))(lambda: kind.first_b(it).start())
        send_y(it)
        for kind in table:
            s_hold = it - LAG_B[3]

            @pl.when(kind.has(s_hold))
            def _():
                kind.back_b(s_hold).wait_recv()
                j = s_hold - kind.begin
                kind.bq[j] = kind.bq[j] + part[s_hold, kind.in_b]

        receive_y(it)
        for kind in table:
            s_go = it - LAG_A[0]
            pl.when(kind.has(s_go))(lambda: kind.first_a(s_go).start())
        s_m = it - LAG_M[0]

        @pl.when(m_has(s_m))
        def _():
            mf, mn = m_first(s_m)
            waits = receive_m(s_m)
            next(waits)
            mf.start()
            next(waits, None)
            mn.start()

        for kind in table:
            gb, ga = kind.gb, kind.ga
            s_a3, s_swap, s_last = it - LAG_A[3], it - LAG_SWAP, it - LAG_X

            @pl.when(kind.has(s_a3))
            def _():
                kind.back_a(s_a3).wait_recv()
                j = s_a3 - kind.begin
                at = pl.multiple_of(kind.base + gb * kind.number + j * ga, 8)
                var_acc[pl.ds(at, ga), :] = square(kind.aq[j] + part[s_a3, kind.in_a])

            pl.when(kind.has(s_swap))(lambda: kind.swap(s_swap).start())

            @pl.when(kind.has(s_last))
            def _():
                kind.swap(s_last).wait_recv()
                j = s_last - kind.begin
                mine = pl.ds(pl.multiple_of(y * gb, 8), gb)
                at = pl.multiple_of(kind.base + j * gb, 8)
                var_acc[pl.ds(at, gb), :] = square(kind.bq[j, mine] + kind.got_x[j])

        means(it)
        return carry

    def middle_turn(it, carry):
        pl.when((it > 0) & (it < steps))(lambda: compute(it))
        send_y(it)
        for kind in table:
            s_1, s_2 = it - LAG_B[1], it - LAG_B[2]

            @pl.when(kind.has(s_1))
            def _():
                kind.first_b(s_1).wait_recv()
                j = s_1 - kind.begin
                kind.bp[j] = kind.bp[j] + part[s_1, kind.out_b]
                kind.cross_b(s_1).start()

            @pl.when(kind.has(s_2))
            def _():
                kind.cross_b(s_2).wait_recv()
                j = s_2 - kind.begin
                kind.bq[j] = kind.bq[j] + part[s_2, kind.in_b]
                kind.back_b(s_2).start()

        receive_y(it)
        s_m = it - LAG_M[0]

        @pl.when(m_has(s_m))
        def _():
            for _ in receive_m(s_m):
                pass

        for kind in table:
            s_1, s_2 = it - LAG_A[1], it - LAG_A[2]

            @pl.when(kind.has(s_1))
            def _():
                kind.first_a(s_1).wait_recv()
                j = s_1 - kind.begin
                kind.ap[j] = kind.ap[j] + part[s_1, kind.out_a]
                kind.cross_a(s_1).start()

            @pl.when(kind.has(s_2))
            def _():
                kind.cross_a(s_2).wait_recv()
                j = s_2 - kind.begin
                kind.aq[j] = kind.aq[j] + part[s_2, kind.in_a]
                kind.back_a(s_2).start()

        s_m1, s_m2 = it - LAG_M[1], it - LAG_M[2]

        @pl.when(m_has(s_m1))
        def _():
            m_first(s_m1)[0].wait_recv()
            j = s_m1 - m_begin
            got_mf[j] = got_mf[j] + part[s_m1, 2 * gm : 3 * gm]
            m_cross(s_m1).start()

        @pl.when(m_has(s_m2))
        def _():
            m_first(s_m2)[1].wait_recv()
            m_cross(s_m2).wait_recv()
            j = s_m2 - m_begin
            at = pl.multiple_of(m_base + j * gm, 8)
            var_acc[pl.ds(at, gm), :] = square(got_mn[j] + part[s_m2, 3 * gm :] + got_mx[j])

        means(it)
        return carry

    def settle_y():
        for kind in table:
            def done(s, carry):
                kind.copy_y(s).wait_send()
                return carry

            lax.fori_loop(kind.begin, kind.begin + kind.number, done, 0)

        for s in range(m_begin, m_begin + m_number):
            for copy in m_y(s):
                copy.wait_send()

    def collect(is_end):
        for k in range(1, LINE):
            mean_copy(k).wait()
        total = mean_box[0]
        for index in range(1, LINE):
            total = total + mean_box[index]
        out_ref[: rows // 128, :] = total
        settle_y()
        for kind in table:
            def done(s, carry):
                if is_end:
                    for copy in (kind.first_b(s), kind.first_a(s), kind.swap(s)):
                        copy.wait_send()
                else:
                    for copy in (kind.cross_b(s), kind.back_b(s), kind.cross_a(s), kind.back_a(s)):
                        copy.wait_send()
                return carry

            lax.fori_loop(kind.begin, kind.begin + kind.number, done, 0)
        for s in range(m_begin, m_begin + m_number):
            for copy in m_first(s) if is_end else (m_cross(s),):
                copy.wait_send()
        for who in range(4):
            if is_end:
                mid_copy(1, who).wait_recv()
                pl.when(owner != who)(lambda: var_copy(1, who).wait_recv())
            else:
                var_copy(1, who).wait_recv()
                pl.when(owner != who)(lambda: mid_copy(1, who).wait_recv())
        for who in range(4):
            begin = rows // 128 + who * lines
            out_ref[begin : begin + lines - 1, :] = 1.0 - var_box[who, : lines - 1]
            out_ref[begin + lines - 1 : begin + lines, :] = 1.0 - (var_box[who, lines - 1 :] + mid_box[who])
        for k in range(1, count):
            (var_copy if is_end else mid_copy)(k, owner).wait_send()

    compute(0, True)
    pl.semaphore_wait(barrier, count - 1)
    total_turns = steps + max(LAG_X, LAG_A[3], LAG_M[2])

    @pl.when(ends)
    def _():
        lax.fori_loop(0, total_turns, end_turn, 0)
        for index in range(lines):
            var_box[owner, index : index + 1, :] = line_of(index)
        for k in range(1, count):
            var_copy(k, owner).start()
        collect(True)

    @pl.when(jnp.logical_not(ends))
    def _():
        lax.fori_loop(0, total_turns, middle_turn, 0)
        mid_box[owner] = line_of(lines - 1)
        for k in range(1, count):
            mid_copy(k, owner).start()
        collect(False)


def fused(test_points, train_points, weights, factor, *, count):
    dim, rows = test_points.shape
    local = train_points.shape[1]
    width = factor.shape[1]
    depth = -(-(dim + 16) // 128) * 128
    steps = rows // BLOCK
    dma = pltpu.SemaphoreType.DMA
    f32 = jnp.float32
    kinds, (_, m_number, gm, _) = kinds_of(rows)
    sems = [dma((steps,))] * 12 + [dma((m_number,))] * 8
    sems += [dma((LINE,)), dma((LINE,)), dma((count,)), dma((4,)), dma((4,))]
    boxes = [pltpu.VMEM((m_number, gm, width), f32)] * 5
    for _, number, gb, ga, _ in kinds:
        for size in (2 * ga, 2 * gb, 2 * gb, ga, ga, gb):
            boxes.append(pltpu.VMEM((number, size, width), f32))
    out = pl.pallas_call(
        functools.partial(kernel, count=count),
        out_shape=jax.ShapeDtypeStruct((rows // 64, 128), f32),
        in_specs=[pl.BlockSpec(memory_space=pl.ANY)] * 4,
        out_specs=pl.BlockSpec(memory_space=pltpu.VMEM),
        scratch_shapes=[
            pltpu.VMEM((dim, rows), jnp.bfloat16),
            pltpu.VMEM((dim, local), jnp.bfloat16),
            pltpu.VMEM((local // 128, 128), jnp.bfloat16),
            pltpu.VMEM((local, width), jnp.bfloat16),
            dma((3 + local // CHUNK,)),
            pltpu.VMEM((rows, depth), f32),
            pltpu.VMEM((depth, local), jnp.bfloat16),
            pltpu.VMEM((1, local), f32),
            pltpu.VMEM((BLOCK, depth), jnp.bfloat16),
            pltpu.VMEM((steps, BLOCK, width), f32),
            pltpu.VMEM((rows, 128), f32),
            pltpu.VMEM((rows // 4, 128), f32),
            pltpu.VMEM((LINE + 1, rows // 128, 128), f32),
            pltpu.VMEM((4, rows // 512, 128), f32),
            pltpu.VMEM((4, 1, 128), f32),
        ] + sems + boxes,
        compiler_params=pltpu.CompilerParams(
            collective_id=0, has_side_effects=True, vmem_limit_bytes=56 * 1024 * 1024
        ),
    )(test_points, train_points, weights.reshape(local // 128, 128), factor)
    lines = rows // 128
    return out[:lines].reshape(rows), out[lines:].reshape(rows)


def on_device(test_points, train_points, weights, factor):
    rows = test_points.shape[1]
    local = train_points.shape[1]
    dim = test_points.shape[0]
    width = factor.shape[1]
    test_sq = jnp.sum(test_points.astype(jnp.float32) ** 2, axis=0)
    block = math.gcd(local, 1024)
    turns = local // block

    def step(index, carry):
        mean_acc, proj_acc = carry
        start = (index * block).astype(jnp.int32)
        points = lax.dynamic_slice_in_dim(train_points, start, block, 1)
        wblock = lax.dynamic_slice_in_dim(weights, start, block, 0)
        fblock = lax.dynamic_slice_in_dim(factor, start, block, 0)
        train_sq = jnp.sum(points.astype(jnp.float32) ** 2, axis=0)
        cross = lax.dot_general(
            test_points, points, (((0,), (0,)), ((), ())), preferred_element_type=jnp.float32
        )
        kernel = jnp.exp(
            -(test_sq[:, None] + train_sq[None, :] - 2.0 * cross) * (4.0 / dim)
        ).astype(jnp.bfloat16)
        mean_acc = mean_acc + jnp.dot(kernel, wblock, preferred_element_type=jnp.float32)
        proj_acc = proj_acc + jnp.dot(kernel, fblock, preferred_element_type=jnp.float32)
        return (mean_acc, proj_acc)

    init = (jnp.zeros((rows,), jnp.float32), jnp.zeros((rows, width), jnp.float32))
    mean_part, proj_part = lax.fori_loop(0, turns, step, init)
    mean_share, proj_share = (
        lax.psum_scatter(mean_part, "trn", scatter_dimension=0, tiled=True),
        lax.psum_scatter(proj_part, "trn", scatter_dimension=0, tiled=True),
    )
    var_share = 1.0 - jnp.sum(proj_share * proj_share, axis=1)
    mean, variance = (
        lax.all_gather(mean_share, "trn", axis=0, tiled=True),
        lax.all_gather(var_share, "trn", axis=0, tiled=True),
    )
    return (mean, variance)


def solution(mesh):
    in_specs = (
        P(None, ("grp", "tst")),
        P(None, ("grp", "trn")),
        P(("grp", "trn")),
        P(("grp", "trn"), None),
    )
    out_specs = (P(("grp", "tst")), P(("grp", "tst")))
    count = mesh.shape["trn"]
    body = functools.partial(fused, count=count) if count == 2 * LINE else on_device
    return jax.shard_map(
        body, mesh=mesh, in_specs=in_specs, out_specs=out_specs, check_vma=False
    )
```

```python
import functools
import math

import jax
import jax.numpy as jnp
from jax import lax
from jax.experimental import pallas as pl
from jax.experimental.pallas import tpu as pltpu
from jax.sharding import PartitionSpec as P

LOG2E = 1.4426950408889634
BLOCK = 128
CHUNK = 1024
LINE = 4
KINDS = ((10, 16, 16), (4, 8, 24))
MIDDLE = 2
LAG_Y = 3
LAG_B = (0, 2, 4, 11)
LAG_A = (3, 5, 8, 18)
LAG_SWAP = 11
LAG_X = 18
LAG_M = (4, 6, 17)
MEAN_AT = 1
MEAN_ON = 4


def pieces(value):
    high = value.astype(jnp.bfloat16).astype(jnp.float32)
    rest = value - high
    middle = rest.astype(jnp.bfloat16).astype(jnp.float32)
    low = (rest - middle).astype(jnp.bfloat16).astype(jnp.float32)
    return high, middle, low


def pick(row, table, default):
    value = default
    for index, entry in table:
        value = jnp.where(row == index, entry, value)
    return value


def kinds_of(rows):
    unit = rows // BLOCK // (MIDDLE + sum(count for count, _, _ in KINDS))
    table, begin, base = [], 0, 0
    for count, gb, ga in KINDS:
        count = count * unit
        table.append((begin, count, gb, ga, base))
        begin += count
        base += count * (gb + ga)
    return tuple(table), (begin, MIDDLE * unit, BLOCK // 4, base)


def kernel(
    test_hbm, train_hbm, weights_hbm, factor_hbm, out_ref,
    test_ref, weights_ref, factor_ref, in_sems,
    test_aug, train_aug, wide, left_ref, part, mean_acc, var_acc, mean_box, var_box, mid_box,
    s_y, r_y, s_b, rp_b, sq_b, rq_b, s_a, rp_a, sq_a, rq_a, s_x, r_x,
    s_yn, r_yn, s_mf, r_mf, s_mn, r_mn, s_mx, r_mx,
    s_mean, r_mean, s_var, r_var, r_mid, got_yf, got_yn, got_mf, got_mn, got_mx, *got, count,
):
    pair = count // LINE
    last = LINE - 1
    me = lax.axis_index("trn")
    z = me // pair
    y = me % pair
    dim, rows = test_ref.shape
    local = train_aug.shape[1]
    depth = test_aug.shape[1]
    steps = rows // BLOCK
    kinds, middle = kinds_of(rows)
    span = rows // 4
    other = z * pair + (1 - y)
    low = z < 2
    toward = jnp.where(low, me + pair, me - pair)
    back = jnp.where(low, me - pair, me + pair)
    far = jnp.where(low, 2, 0)
    near = 2 - far
    owner = near + y
    ends = (z == 0) | (z == last)
    chunks = local // CHUNK

    barrier = pltpu.get_barrier_semaphore()
    for k in range(1, count):
        pl.semaphore_signal(barrier, inc=1, device_id={"trn": lax.rem(me + k, count)})

    def fetch(index, source, target):
        return pltpu.make_async_copy(source, target, in_sems.at[index])

    fetch_train = fetch(0, train_hbm, train_aug.at[:dim])
    fetch_test = fetch(1, test_hbm, test_ref)
    fetch_weights = fetch(2, weights_hbm, weights_ref)

    def fetch_factor(index):
        block = pl.ds(index * CHUNK, CHUNK)
        return fetch(3 + index, factor_hbm.at[block], factor_ref.at[block])

    fetch_train.start()
    fetch_test.start()
    fetch_weights.start()
    for index in range(chunks):
        fetch_factor(index).start()

    var_acc[...] = jnp.zeros_like(var_acc)
    train_aug[dim + 16 :, :] = jnp.zeros((depth - dim - 16, local), jnp.bfloat16)
    fetch_train.wait()

    def prepare_train(index, carry):
        cols = pl.ds(pl.multiple_of(index * 512, 512), 512)
        points = train_aug[:dim, cols]
        squares = points.astype(jnp.float32) ** 2
        norm = jnp.sum(squares, axis=0, keepdims=True) * (-4.0 / dim)
        high, middle, low = pieces(norm)
        row = lax.broadcasted_iota(jnp.int32, (16, 512), 0)
        one = jnp.float32(1.0)
        extra = pick(row, ((0, one), (1, one), (2, one), (3, high), (4, middle), (5, low)), jnp.float32(0.0))
        train_aug[dim : dim + 16, cols] = extra.astype(jnp.bfloat16)
        return carry

    lax.fori_loop(0, local // 512, prepare_train, 0, unroll=True)
    fetch_test.wait()

    def prepare_test(index, carry):
        cols = pl.ds(pl.multiple_of(index * 256, 256), 256)
        points = test_ref[:, cols].astype(jnp.float32)
        norm = jnp.sum(points * points, axis=0, keepdims=True) * (-4.0 / dim)
        high, middle, low = pieces(norm)
        row = lax.broadcasted_iota(jnp.int32, (8, 256), 0)
        one = jnp.float32(1.0)
        extra = pick(row, ((0, high), (1, middle), (2, low), (3, one), (4, one), (5, one)), jnp.float32(0.0))
        whole = jnp.concatenate(
            [points * (8.0 / dim), extra, jnp.zeros((depth - dim - 8, 256), jnp.float32)], axis=0
        )
        test_aug[cols, :] = whole.T
        return carry

    lax.fori_loop(0, rows // 256, prepare_test, 0)
    fetch_weights.wait()
    for index in range(local // 128):
        wide[:, index * 128 : (index + 1) * 128] = weights_ref[index : index + 1, :].astype(jnp.float32)

    def edge_places(kind, step):
        begin, number, gb, ga, base = kind
        index = step - begin

        def row_of(who, early):
            inner = base + (number * gb + index * ga if early else index * gb)
            return pl.multiple_of(who * span + inner, 8)

        where = (
            row_of(far, False), row_of(far + 1, False), row_of(near, False), row_of(near + 1, False),
            row_of(far + 1 - y, True), row_of(near + 1 - y, True), row_of(far + y, True), row_of(near + y, True),
        )
        return tuple(zip(where, (gb,) * 4 + (ga,) * 4))

    def middle_places(step):
        begin, _, gm, base = middle
        inner = base + (step - begin) * gm
        who = (far + 1 - y, near + 1 - y, far + y, near + y)
        return tuple((pl.multiple_of(w * span + inner, 8), gm) for w in who)

    layouts = [(kind[0], kind[1], functools.partial(edge_places, kind)) for kind in kinds]
    layouts.append((middle[0], middle[1], middle_places))

    def compute(step, first=False):
        for begin, number, places in layouts:
            if first and begin > 0:
                continue

            def gather():
                left_ref[...] = jnp.concatenate(
                    [test_aug[pl.ds(at, size), :] for at, size in places(step)], axis=0
                ).astype(jnp.bfloat16)

            if first:
                gather()
            else:
                pl.when((step >= begin) & (step < begin + number))(gather)
        left = left_ref[...]
        total = None
        means = None
        for index in range(chunks):
            begin = index * CHUNK
            power = jnp.dot(
                left, train_aug[:, begin : begin + CHUNK], preferred_element_type=jnp.float32
            )
            values = jnp.exp2(power * LOG2E).astype(jnp.bfloat16)
            scaled = values.astype(jnp.float32) * wide[:, begin : begin + CHUNK]
            for lane in range(0, CHUNK, 128):
                piece = scaled[:, lane : lane + 128]
                means = piece if means is None else means + piece
            product = jnp.dot(
                values, factor_ref[begin : begin + CHUNK, :], preferred_element_type=jnp.float32
            )
            total = product if total is None else total + product
        part[step] = total
        mean_acc[pl.ds(pl.multiple_of(step * BLOCK, BLOCK), BLOCK), :] = means

    def send(source, target, ssem, rsem, device):
        return pltpu.make_async_remote_copy(
            src_ref=source, dst_ref=target, send_sem=ssem, recv_sem=rsem, device_id={"trn": device}
        )

    def square(values):
        total = None
        for lane in range(0, values.shape[1], 128):
            piece = values[:, lane : lane + 128]
            total = piece * piece if total is None else total + piece * piece
        return total

    class Kind:
        def __init__(self, kind, buffers):
            self.begin, self.number, self.gb, self.ga, self.base = kind
            self.got_y, self.bp, self.bq, self.ap, self.aq, self.got_x = buffers
            gb, ga = self.gb, self.ga
            self.sent = slice(4 * gb, 4 * gb + 2 * ga)
            self.kept = slice(4 * gb + 2 * ga, 4 * gb + 4 * ga)
            self.out_b, self.in_b = slice(0, 2 * gb), slice(2 * gb, 4 * gb)
            self.out_a = slice(4 * gb + 2 * ga, 4 * gb + 3 * ga)
            self.in_a = slice(4 * gb + 3 * ga, 4 * gb + 4 * ga)

        def has(self, s):
            return (s >= self.begin) & (s < self.begin + self.number)

        def copy_y(self, s):
            return send(part.at[s, self.sent], self.got_y.at[s - self.begin], s_y.at[s], r_y.at[s], other)

        def first_b(self, s):
            return send(part.at[s, self.out_b], self.bp.at[s - self.begin], s_b.at[s], rp_b.at[s], toward)

        def cross_b(self, s):
            j = s - self.begin
            return send(self.bp.at[j], self.bq.at[j], s_b.at[s], rq_b.at[s], toward)

        def back_b(self, s):
            j = s - self.begin
            return send(self.bq.at[j], self.bq.at[j], sq_b.at[s], rq_b.at[s], back)

        def first_a(self, s):
            return send(part.at[s, self.out_a], self.ap.at[s - self.begin], s_a.at[s], rp_a.at[s], toward)

        def cross_a(self, s):
            j = s - self.begin
            return send(self.ap.at[j], self.aq.at[j], s_a.at[s], rq_a.at[s], toward)

        def back_a(self, s):
            j = s - self.begin
            return send(self.aq.at[j], self.aq.at[j], sq_a.at[s], rq_a.at[s], back)

        def swap(self, s):
            j = s - self.begin
            theirs = pl.ds(pl.multiple_of((1 - y) * self.gb, 8), self.gb)
            return send(self.bq.at[j, theirs], self.got_x.at[j], s_x.at[s], r_x.at[s], other)

    table = [Kind(kind, got[6 * i : 6 * i + 6]) for i, kind in enumerate(kinds)]
    m_begin, m_number, gm, m_base = middle

    def m_has(s):
        return (s >= m_begin) & (s < m_begin + m_number)

    def m_y(s):
        j = s - m_begin
        return (
            send(part.at[s, :gm], got_yf.at[j], s_y.at[s], r_y.at[s], other),
            send(part.at[s, gm : 2 * gm], got_yn.at[j], s_yn.at[j], r_yn.at[j], other),
        )

    def m_first(s):
        j = s - m_begin
        return (
            send(part.at[s, 2 * gm : 3 * gm], got_mf.at[j], s_mf.at[j], r_mf.at[j], toward),
            send(part.at[s, 3 * gm :], got_mn.at[j], s_mn.at[j], r_mn.at[j], toward),
        )

    def m_cross(s):
        j = s - m_begin
        return send(got_mf.at[j], got_mx.at[j], s_mx.at[j], r_mx.at[j], toward)

    def mean_swap():
        return send(mean_box.at[z], mean_box.at[LINE], s_mean.at[0], r_mean.at[0], other)

    def mean_copy(k):
        target = lax.rem(me + k * pair, count)
        return send(mean_box.at[z], mean_box.at[z], s_mean.at[k], r_mean.at[k], target)

    def mean_start():
        for begin, number, places in layouts:
            def place(step, carry):
                start = pl.multiple_of(step * BLOCK, BLOCK)
                for at, size in places(step):
                    test_aug[pl.ds(at, size), :] = mean_acc[pl.ds(start, size), :]
                    start = pl.multiple_of(start + size, 8)
                return carry

            lax.fori_loop(begin, begin + number, place, 0)
        for index in range(rows // 128):
            block = test_aug[index * 128 : (index + 1) * 128, :]
            mean_box[z, index : index + 1, :] = jnp.sum(block.T, axis=0, keepdims=True)
        mean_swap().start()

    def mean_spread():
        mean_swap().wait()
        mean_box[z] = mean_box[z] + mean_box[LINE]
        for k in range(1, LINE):
            mean_copy(k).start()

    lines = span // 128

    def line_of(index):
        block = var_acc[index * 128 : (index + 1) * 128, :]
        return jnp.sum(block.T, axis=0, keepdims=True)

    def var_copy(k, who):
        return send(var_box.at[who], var_box.at[who], s_var.at[k], r_var.at[who], lax.rem(me + k, count))

    def mid_copy(k, who):
        return send(mid_box.at[who], mid_box.at[who], s_var.at[k], r_mid.at[who], lax.rem(me + k, count))

    def receive_y(it):
        for kind in table:
            s = it - LAG_Y

            @pl.when(kind.has(s))
            def _():
                kind.copy_y(s).wait_recv()
                part[s, kind.kept] = part[s, kind.kept] + kind.got_y[s - kind.begin]

    def receive_m(s):
        j = s - m_begin
        yf, yn = m_y(s)
        yf.wait_recv()
        part[s, 2 * gm : 3 * gm] = part[s, 2 * gm : 3 * gm] + got_yf[j]
        yield
        yn.wait_recv()
        part[s, 3 * gm :] = part[s, 3 * gm :] + got_yn[j]

    def send_y(it):
        for kind in table:
            pl.when(kind.has(it))(lambda: kind.copy_y(it).start())

        @pl.when(m_has(it))
        def _():
            for copy in m_y(it):
                copy.start()

    def means(it):
        pl.when(it == steps + MEAN_AT)(mean_start)
        pl.when(it == steps + MEAN_ON)(mean_spread)

    def end_turn(it, carry):
        pl.when((it > 0) & (it < steps))(lambda: compute(it))
        for kind in table:
            pl.when(kind.has(it))(lambda: kind.first_b(it).start())
        send_y(it)
        for kind in table:
            s_hold = it - LAG_B[3]

            @pl.when(kind.has(s_hold))
            def _():
                kind.back_b(s_hold).wait_recv()
                j = s_hold - kind.begin
                kind.bq[j] = kind.bq[j] + part[s_hold, kind.in_b]

        receive_y(it)
        for kind in table:
            s_go = it - LAG_A[0]
            pl.when(kind.has(s_go))(lambda: kind.first_a(s_go).start())
        s_m = it - LAG_M[0]

        @pl.when(m_has(s_m))
        def _():
            mf, mn = m_first(s_m)
            waits = receive_m(s_m)
            next(waits)
            mf.start()
            next(waits, None)
            mn.start()

        for kind in table:
            gb, ga = kind.gb, kind.ga
            s_a3, s_swap, s_last = it - LAG_A[3], it - LAG_SWAP, it - LAG_X

            @pl.when(kind.has(s_a3))
            def _():
                kind.back_a(s_a3).wait_recv()
                j = s_a3 - kind.begin
                at = pl.multiple_of(kind.base + gb * kind.number + j * ga, 8)
                var_acc[pl.ds(at, ga), :] = square(kind.aq[j] + part[s_a3, kind.in_a])

            pl.when(kind.has(s_swap))(lambda: kind.swap(s_swap).start())

            @pl.when(kind.has(s_last))
            def _():
                kind.swap(s_last).wait_recv()
                j = s_last - kind.begin
                mine = pl.ds(pl.multiple_of(y * gb, 8), gb)
                at = pl.multiple_of(kind.base + j * gb, 8)
                var_acc[pl.ds(at, gb), :] = square(kind.bq[j, mine] + kind.got_x[j])

        means(it)
        return carry

    def middle_turn(it, carry):
        pl.when((it > 0) & (it < steps))(lambda: compute(it))
        send_y(it)
        for kind in table:
            s_1, s_2 = it - LAG_B[1], it - LAG_B[2]

            @pl.when(kind.has(s_1))
            def _():
                kind.first_b(s_1).wait_recv()
                j = s_1 - kind.begin
                kind.bp[j] = kind.bp[j] + part[s_1, kind.out_b]
                kind.cross_b(s_1).start()

            @pl.when(kind.has(s_2))
            def _():
                kind.cross_b(s_2).wait_recv()
                j = s_2 - kind.begin
                kind.bq[j] = kind.bq[j] + part[s_2, kind.in_b]
                kind.back_b(s_2).start()

        receive_y(it)
        s_m = it - LAG_M[0]

        @pl.when(m_has(s_m))
        def _():
            for _ in receive_m(s_m):
                pass

        for kind in table:
            s_1, s_2 = it - LAG_A[1], it - LAG_A[2]

            @pl.when(kind.has(s_1))
            def _():
                kind.first_a(s_1).wait_recv()
                j = s_1 - kind.begin
                kind.ap[j] = kind.ap[j] + part[s_1, kind.out_a]
                kind.cross_a(s_1).start()

            @pl.when(kind.has(s_2))
            def _():
                kind.cross_a(s_2).wait_recv()
                j = s_2 - kind.begin
                kind.aq[j] = kind.aq[j] + part[s_2, kind.in_a]
                kind.back_a(s_2).start()

        s_m1, s_m2 = it - LAG_M[1], it - LAG_M[2]

        @pl.when(m_has(s_m1))
        def _():
            m_first(s_m1)[0].wait_recv()
            j = s_m1 - m_begin
            got_mf[j] = got_mf[j] + part[s_m1, 2 * gm : 3 * gm]
            m_cross(s_m1).start()

        @pl.when(m_has(s_m2))
        def _():
            m_first(s_m2)[1].wait_recv()
            m_cross(s_m2).wait_recv()
            j = s_m2 - m_begin
            at = pl.multiple_of(m_base + j * gm, 8)
            var_acc[pl.ds(at, gm), :] = square(got_mn[j] + part[s_m2, 3 * gm :] + got_mx[j])

        means(it)
        return carry

    def settle_y():
        for kind in table:
            def done(s, carry):
                kind.copy_y(s).wait_send()
                return carry

            lax.fori_loop(kind.begin, kind.begin + kind.number, done, 0)

        for s in range(m_begin, m_begin + m_number):
            for copy in m_y(s):
                copy.wait_send()

    def collect(is_end):
        for k in range(1, LINE):
            mean_copy(k).wait()
        total = mean_box[0]
        for index in range(1, LINE):
            total = total + mean_box[index]
        out_ref[: rows // 128, :] = total
        settle_y()
        for kind in table:
            def done(s, carry):
                if is_end:
                    for copy in (kind.first_b(s), kind.first_a(s), kind.swap(s)):
                        copy.wait_send()
                else:
                    for copy in (kind.cross_b(s), kind.back_b(s), kind.cross_a(s), kind.back_a(s)):
                        copy.wait_send()
                return carry

            lax.fori_loop(kind.begin, kind.begin + kind.number, done, 0)
        for s in range(m_begin, m_begin + m_number):
            for copy in m_first(s) if is_end else (m_cross(s),):
                copy.wait_send()
        for who in range(4):
            if is_end:
                mid_copy(1, who).wait_recv()
                pl.when(owner != who)(lambda: var_copy(1, who).wait_recv())
            else:
                var_copy(1, who).wait_recv()
                pl.when(owner != who)(lambda: mid_copy(1, who).wait_recv())
        for who in range(4):
            begin = rows // 128 + who * lines
            out_ref[begin : begin + lines - 1, :] = 1.0 - var_box[who, : lines - 1]
            out_ref[begin + lines - 1 : begin + lines, :] = 1.0 - (var_box[who, lines - 1 :] + mid_box[who])
        for k in range(1, count):
            (var_copy if is_end else mid_copy)(k, owner).wait_send()

    for index in range(chunks):
        fetch_factor(index).wait()
    compute(0, True)
    pl.semaphore_wait(barrier, count - 1)
    total_turns = steps + max(LAG_X, LAG_A[3], LAG_M[2])

    @pl.when(ends)
    def _():
        lax.fori_loop(0, total_turns, end_turn, 0)
        for index in range(lines):
            var_box[owner, index : index + 1, :] = line_of(index)
        for k in range(1, count):
            var_copy(k, owner).start()
        collect(True)

    @pl.when(jnp.logical_not(ends))
    def _():
        lax.fori_loop(0, total_turns, middle_turn, 0)
        mid_box[owner] = line_of(lines - 1)
        for k in range(1, count):
            mid_copy(k, owner).start()
        collect(False)


def fused(test_points, train_points, weights, factor, *, count):
    dim, rows = test_points.shape
    local = train_points.shape[1]
    width = factor.shape[1]
    depth = -(-(dim + 16) // 128) * 128
    steps = rows // BLOCK
    dma = pltpu.SemaphoreType.DMA
    f32 = jnp.float32
    kinds, (_, m_number, gm, _) = kinds_of(rows)
    sems = [dma((steps,))] * 12 + [dma((m_number,))] * 8
    sems += [dma((LINE,)), dma((LINE,)), dma((count,)), dma((4,)), dma((4,))]
    boxes = [pltpu.VMEM((m_number, gm, width), f32)] * 5
    for _, number, gb, ga, _ in kinds:
        for size in (2 * ga, 2 * gb, 2 * gb, ga, ga, gb):
            boxes.append(pltpu.VMEM((number, size, width), f32))
    out = pl.pallas_call(
        functools.partial(kernel, count=count),
        out_shape=pltpu.VMEM((rows // 64, 128), f32),
        in_specs=[pl.BlockSpec(memory_space=pl.ANY)] * 4,
        out_specs=pl.BlockSpec(memory_space=pltpu.VMEM),
        scratch_shapes=[
            pltpu.VMEM((dim, rows), jnp.bfloat16),
            pltpu.VMEM((local // 128, 128), jnp.bfloat16),
            pltpu.VMEM((local, width), jnp.bfloat16),
            dma((3 + local // CHUNK,)),
            pltpu.VMEM((rows, depth), f32),
            pltpu.VMEM((depth, local), jnp.bfloat16),
            pltpu.VMEM((1, local), f32),
            pltpu.VMEM((BLOCK, depth), jnp.bfloat16),
            pltpu.VMEM((steps, BLOCK, width), f32),
            pltpu.VMEM((rows, 128), f32),
            pltpu.VMEM((rows // 4, 128), f32),
            pltpu.VMEM((LINE + 1, rows // 128, 128), f32),
            pltpu.VMEM((4, rows // 512, 128), f32),
            pltpu.VMEM((4, 1, 128), f32),
        ] + sems + boxes,
        compiler_params=pltpu.CompilerParams(
            collective_id=0, has_side_effects=True, vmem_limit_bytes=40 * 1024 * 1024
        ),
    )(*[pltpu.with_memory_space_constraint(x, pltpu.HBM) for x in (test_points, train_points, weights.reshape(local // 128, 128), factor)])
    lines = rows // 128
    return out[:lines].reshape(rows), out[lines:].reshape(rows)


def on_device(test_points, train_points, weights, factor):
    rows = test_points.shape[1]
    local = train_points.shape[1]
    dim = test_points.shape[0]
    width = factor.shape[1]
    test_sq = jnp.sum(test_points.astype(jnp.float32) ** 2, axis=0)
    block = math.gcd(local, 1024)
    turns = local // block

    def step(index, carry):
        mean_acc, proj_acc = carry
        start = (index * block).astype(jnp.int32)
        points = lax.dynamic_slice_in_dim(train_points, start, block, 1)
        wblock = lax.dynamic_slice_in_dim(weights, start, block, 0)
        fblock = lax.dynamic_slice_in_dim(factor, start, block, 0)
        train_sq = jnp.sum(points.astype(jnp.float32) ** 2, axis=0)
        cross = lax.dot_general(
            test_points, points, (((0,), (0,)), ((), ())), preferred_element_type=jnp.float32
        )
        kernel = jnp.exp(
            -(test_sq[:, None] + train_sq[None, :] - 2.0 * cross) * (4.0 / dim)
        ).astype(jnp.bfloat16)
        mean_acc = mean_acc + jnp.dot(kernel, wblock, preferred_element_type=jnp.float32)
        proj_acc = proj_acc + jnp.dot(kernel, fblock, preferred_element_type=jnp.float32)
        return (mean_acc, proj_acc)

    init = (jnp.zeros((rows,), jnp.float32), jnp.zeros((rows, width), jnp.float32))
    mean_part, proj_part = lax.fori_loop(0, turns, step, init)
    mean_share, proj_share = (
        lax.psum_scatter(mean_part, "trn", scatter_dimension=0, tiled=True),
        lax.psum_scatter(proj_part, "trn", scatter_dimension=0, tiled=True),
    )
    var_share = 1.0 - jnp.sum(proj_share * proj_share, axis=1)
    mean, variance = (
        lax.all_gather(mean_share, "trn", axis=0, tiled=True),
        lax.all_gather(var_share, "trn", axis=0, tiled=True),
    )
    return (mean, variance)


def solution(mesh):
    in_specs = (
        P(None, ("grp", "tst")),
        P(None, ("grp", "trn")),
        P(("grp", "trn")),
        P(("grp", "trn"), None),
    )
    out_specs = (P(("grp", "tst")), P(("grp", "tst")))
    count = mesh.shape["trn"]
    body = functools.partial(fused, count=count) if count == 2 * LINE else on_device
    return jax.shard_map(
        body, mesh=mesh, in_specs=in_specs, out_specs=out_specs, check_vma=False
    )
```

```python
import functools
import math

import jax
import jax.numpy as jnp
from jax import lax
from jax.experimental import pallas as pl
from jax.experimental.pallas import tpu as pltpu
from jax.sharding import PartitionSpec as P

LOG2E = 1.4426950408889634
BLOCK = 128
CHUNK = 1024
LINE = 4
KINDS = ((10, 16, 16), (4, 8, 24))
MIDDLE = 2
LAG_Y = 3
LAG_B = (0, 2, 4, 11)
LAG_A = (3, 5, 8, 18)
LAG_SWAP = 11
LAG_X = 18
LAG_M = (4, 6, 17)
MEAN_AT = 1
MEAN_ON = 4


def pieces(value):
    high = value.astype(jnp.bfloat16).astype(jnp.float32)
    rest = value - high
    middle = rest.astype(jnp.bfloat16).astype(jnp.float32)
    low = (rest - middle).astype(jnp.bfloat16).astype(jnp.float32)
    return high, middle, low


def pick(row, table, default):
    value = default
    for index, entry in table:
        value = jnp.where(row == index, entry, value)
    return value


def kinds_of(rows):
    unit = rows // BLOCK // (MIDDLE + sum(count for count, _, _ in KINDS))
    table, begin, base = [], 0, 0
    for count, gb, ga in KINDS:
        count = count * unit
        table.append((begin, count, gb, ga, base))
        begin += count
        base += count * (gb + ga)
    return tuple(table), (begin, MIDDLE * unit, BLOCK // 4, base)


def kernel(
    test_hbm, train_hbm, weights_hbm, factor_hbm, out_ref,
    test_ref, weights_ref, factor_ref, in_sems,
    test_aug, train_aug, wide, left_ref, part, mean_acc, var_acc, mean_box, var_box, mid_box,
    s_y, r_y, s_b, rp_b, sq_b, rq_b, s_a, rp_a, sq_a, rq_a, s_x, r_x,
    s_yn, r_yn, s_mf, r_mf, s_mn, r_mn, s_mx, r_mx,
    s_mean, r_mean, s_var, r_var, r_mid, got_yf, got_yn, got_mf, got_mn, got_mx, *got, count,
):
    pair = count // LINE
    last = LINE - 1
    me = lax.axis_index("trn")
    z = me // pair
    y = me % pair
    dim, rows = test_ref.shape
    local = train_aug.shape[1]
    depth = test_aug.shape[1]
    steps = rows // BLOCK
    kinds, middle = kinds_of(rows)
    span = rows // 4
    other = z * pair + (1 - y)
    low = z < 2
    toward = jnp.where(low, me + pair, me - pair)
    back = jnp.where(low, me - pair, me + pair)
    far = jnp.where(low, 2, 0)
    near = 2 - far
    owner = near + y
    ends = (z == 0) | (z == last)
    chunks = local // CHUNK

    def fetch(index, source, target):
        return pltpu.make_async_copy(source, target, in_sems.at[index])

    fetch_train = fetch(0, train_hbm, train_aug.at[:dim])
    fetch_test = fetch(1, test_hbm, test_ref)
    fetch_weights = fetch(2, weights_hbm, weights_ref)

    def fetch_factor(index):
        block = pl.ds(index * CHUNK, CHUNK)
        return fetch(3 + index, factor_hbm.at[block], factor_ref.at[block])

    fetch_train.start()
    fetch_test.start()
    fetch_weights.start()
    for index in range(chunks):
        fetch_factor(index).start()

    barrier = pltpu.get_barrier_semaphore()
    for k in range(1, count):
        pl.semaphore_signal(barrier, inc=1, device_id={"trn": lax.rem(me + k, count)})

    var_acc[...] = jnp.zeros_like(var_acc)
    train_aug[dim + 16 :, :] = jnp.zeros((depth - dim - 16, local), jnp.bfloat16)
    fetch_train.wait()

    def prepare_train(index, carry):
        cols = pl.ds(pl.multiple_of(index * 512, 512), 512)
        points = train_aug[:dim, cols]
        squares = points.astype(jnp.float32) ** 2
        norm = jnp.sum(squares, axis=0, keepdims=True) * (-4.0 / dim)
        high, middle, low = pieces(norm)
        row = lax.broadcasted_iota(jnp.int32, (16, 512), 0)
        one = jnp.float32(1.0)
        extra = pick(row, ((0, one), (1, one), (2, one), (3, high), (4, middle), (5, low)), jnp.float32(0.0))
        train_aug[dim : dim + 16, cols] = extra.astype(jnp.bfloat16)
        return carry

    lax.fori_loop(0, local // 512, prepare_train, 0, unroll=True)
    fetch_test.wait()

    def prepare_test(index, carry):
        cols = pl.ds(pl.multiple_of(index * 256, 256), 256)
        points = test_ref[:, cols].astype(jnp.float32)
        norm = jnp.sum(points * points, axis=0, keepdims=True) * (-4.0 / dim)
        high, middle, low = pieces(norm)
        row = lax.broadcasted_iota(jnp.int32, (8, 256), 0)
        one = jnp.float32(1.0)
        extra = pick(row, ((0, high), (1, middle), (2, low), (3, one), (4, one), (5, one)), jnp.float32(0.0))
        whole = jnp.concatenate(
            [points * (8.0 / dim), extra, jnp.zeros((depth - dim - 8, 256), jnp.float32)], axis=0
        )
        test_aug[cols, :] = whole.T
        return carry

    lax.fori_loop(0, rows // 256, prepare_test, 0, unroll=True)
    fetch_weights.wait()
    for index in range(local // 128):
        wide[:, index * 128 : (index + 1) * 128] = weights_ref[index : index + 1, :].astype(jnp.float32)

    def edge_places(kind, step):
        begin, number, gb, ga, base = kind
        index = step - begin

        def row_of(who, early):
            inner = base + (number * gb + index * ga if early else index * gb)
            return pl.multiple_of(who * span + inner, 8)

        where = (
            row_of(far, False), row_of(far + 1, False), row_of(near, False), row_of(near + 1, False),
            row_of(far + 1 - y, True), row_of(near + 1 - y, True), row_of(far + y, True), row_of(near + y, True),
        )
        return tuple(zip(where, (gb,) * 4 + (ga,) * 4))

    def middle_places(step):
        begin, _, gm, base = middle
        inner = base + (step - begin) * gm
        who = (far + 1 - y, near + 1 - y, far + y, near + y)
        return tuple((pl.multiple_of(w * span + inner, 8), gm) for w in who)

    layouts = [(kind[0], kind[1], functools.partial(edge_places, kind)) for kind in kinds]
    layouts.append((middle[0], middle[1], middle_places))

    def compute(step, first=False):
        for begin, number, places in layouts:
            if first and begin > 0:
                continue

            def gather():
                left_ref[...] = jnp.concatenate(
                    [test_aug[pl.ds(at, size), :] for at, size in places(step)], axis=0
                ).astype(jnp.bfloat16)

            if first:
                gather()
            else:
                pl.when((step >= begin) & (step < begin + number))(gather)
        left = left_ref[...]
        total = None
        means = None
        held = []
        for index in range(chunks):
            begin = index * CHUNK
            power = jnp.dot(
                left, train_aug[:, begin : begin + CHUNK], preferred_element_type=jnp.float32
            )
            values = jnp.exp2(power * LOG2E).astype(jnp.bfloat16)
            scaled = values.astype(jnp.float32) * wide[:, begin : begin + CHUNK]
            for lane in range(0, CHUNK, 128):
                piece = scaled[:, lane : lane + 128]
                means = piece if means is None else means + piece
            if first:
                held.append(values)
                continue
            product = jnp.dot(
                values, factor_ref[begin : begin + CHUNK, :], preferred_element_type=jnp.float32
            )
            total = product if total is None else total + product
        if first:
            for index in range(chunks):
                fetch_factor(index).wait()
            total = jnp.dot(
                jnp.concatenate(held, axis=1), factor_ref[...], preferred_element_type=jnp.float32
            )
        part[step] = total
        mean_acc[pl.ds(pl.multiple_of(step * BLOCK, BLOCK), BLOCK), :] = means

    def send(source, target, ssem, rsem, device):
        return pltpu.make_async_remote_copy(
            src_ref=source, dst_ref=target, send_sem=ssem, recv_sem=rsem, device_id={"trn": device}
        )

    def square(values):
        total = None
        for lane in range(0, values.shape[1], 128):
            piece = values[:, lane : lane + 128]
            total = piece * piece if total is None else total + piece * piece
        return total

    class Kind:
        def __init__(self, kind, buffers):
            self.begin, self.number, self.gb, self.ga, self.base = kind
            self.got_y, self.bp, self.bq, self.ap, self.aq, self.got_x = buffers
            gb, ga = self.gb, self.ga
            self.sent = slice(4 * gb, 4 * gb + 2 * ga)
            self.kept = slice(4 * gb + 2 * ga, 4 * gb + 4 * ga)
            self.out_b, self.in_b = slice(0, 2 * gb), slice(2 * gb, 4 * gb)
            self.out_a = slice(4 * gb + 2 * ga, 4 * gb + 3 * ga)
            self.in_a = slice(4 * gb + 3 * ga, 4 * gb + 4 * ga)

        def has(self, s):
            return (s >= self.begin) & (s < self.begin + self.number)

        def copy_y(self, s):
            return send(part.at[s, self.sent], self.got_y.at[s - self.begin], s_y.at[s], r_y.at[s], other)

        def first_b(self, s):
            return send(part.at[s, self.out_b], self.bp.at[s - self.begin], s_b.at[s], rp_b.at[s], toward)

        def cross_b(self, s):
            j = s - self.begin
            return send(self.bp.at[j], self.bq.at[j], s_b.at[s], rq_b.at[s], toward)

        def back_b(self, s):
            j = s - self.begin
            return send(self.bq.at[j], self.bq.at[j], sq_b.at[s], rq_b.at[s], back)

        def first_a(self, s):
            return send(part.at[s, self.out_a], self.ap.at[s - self.begin], s_a.at[s], rp_a.at[s], toward)

        def cross_a(self, s):
            j = s - self.begin
            return send(self.ap.at[j], self.aq.at[j], s_a.at[s], rq_a.at[s], toward)

        def back_a(self, s):
            j = s - self.begin
            return send(self.aq.at[j], self.aq.at[j], sq_a.at[s], rq_a.at[s], back)

        def swap(self, s):
            j = s - self.begin
            theirs = pl.ds(pl.multiple_of((1 - y) * self.gb, 8), self.gb)
            return send(self.bq.at[j, theirs], self.got_x.at[j], s_x.at[s], r_x.at[s], other)

    table = [Kind(kind, got[6 * i : 6 * i + 6]) for i, kind in enumerate(kinds)]
    m_begin, m_number, gm, m_base = middle

    def m_has(s):
        return (s >= m_begin) & (s < m_begin + m_number)

    def m_y(s):
        j = s - m_begin
        return (
            send(part.at[s, :gm], got_yf.at[j], s_y.at[s], r_y.at[s], other),
            send(part.at[s, gm : 2 * gm], got_yn.at[j], s_yn.at[j], r_yn.at[j], other),
        )

    def m_first(s):
        j = s - m_begin
        return (
            send(part.at[s, 2 * gm : 3 * gm], got_mf.at[j], s_mf.at[j], r_mf.at[j], toward),
            send(part.at[s, 3 * gm :], got_mn.at[j], s_mn.at[j], r_mn.at[j], toward),
        )

    def m_cross(s):
        j = s - m_begin
        return send(got_mf.at[j], got_mx.at[j], s_mx.at[j], r_mx.at[j], toward)

    def mean_swap():
        return send(mean_box.at[z], mean_box.at[LINE], s_mean.at[0], r_mean.at[0], other)

    def mean_copy(k):
        target = lax.rem(me + k * pair, count)
        return send(mean_box.at[z], mean_box.at[z], s_mean.at[k], r_mean.at[k], target)

    def mean_start():
        for begin, number, places in layouts:
            def place(step, carry):
                start = pl.multiple_of(step * BLOCK, BLOCK)
                for at, size in places(step):
                    test_aug[pl.ds(at, size), :] = mean_acc[pl.ds(start, size), :]
                    start = pl.multiple_of(start + size, 8)
                return carry

            lax.fori_loop(begin, begin + number, place, 0)
        for index in range(rows // 128):
            block = test_aug[index * 128 : (index + 1) * 128, :]
            mean_box[z, index : index + 1, :] = jnp.sum(block.T, axis=0, keepdims=True)
        mean_swap().start()

    def mean_spread():
        mean_swap().wait()
        mean_box[z] = mean_box[z] + mean_box[LINE]
        for k in range(1, LINE):
            mean_copy(k).start()

    lines = span // 128

    def line_of(index):
        block = var_acc[index * 128 : (index + 1) * 128, :]
        return jnp.sum(block.T, axis=0, keepdims=True)

    def var_copy(k, who):
        return send(var_box.at[who], var_box.at[who], s_var.at[k], r_var.at[who], lax.rem(me + k, count))

    def mid_copy(k, who):
        return send(mid_box.at[who], mid_box.at[who], s_var.at[k], r_mid.at[who], lax.rem(me + k, count))

    def receive_y(it):
        for kind in table:
            s = it - LAG_Y

            @pl.when(kind.has(s))
            def _():
                kind.copy_y(s).wait_recv()
                part[s, kind.kept] = part[s, kind.kept] + kind.got_y[s - kind.begin]

    def receive_m(s):
        j = s - m_begin
        yf, yn = m_y(s)
        yf.wait_recv()
        part[s, 2 * gm : 3 * gm] = part[s, 2 * gm : 3 * gm] + got_yf[j]
        yield
        yn.wait_recv()
        part[s, 3 * gm :] = part[s, 3 * gm :] + got_yn[j]

    def send_y(it):
        for kind in table:
            pl.when(kind.has(it))(lambda: kind.copy_y(it).start())

        @pl.when(m_has(it))
        def _():
            for copy in m_y(it):
                copy.start()

    def means(it):
        pl.when(it == steps + MEAN_AT)(mean_start)
        pl.when(it == steps + MEAN_ON)(mean_spread)

    def end_turn(it, carry):
        pl.when((it > 0) & (it < steps))(lambda: compute(it))
        for kind in table:
            pl.when(kind.has(it))(lambda: kind.first_b(it).start())
        send_y(it)
        for kind in table:
            s_hold = it - LAG_B[3]

            @pl.when(kind.has(s_hold))
            def _():
                kind.back_b(s_hold).wait_recv()
                j = s_hold - kind.begin
                kind.bq[j] = kind.bq[j] + part[s_hold, kind.in_b]

        receive_y(it)
        for kind in table:
            s_go = it - LAG_A[0]
            pl.when(kind.has(s_go))(lambda: kind.first_a(s_go).start())
        s_m = it - LAG_M[0]

        @pl.when(m_has(s_m))
        def _():
            mf, mn = m_first(s_m)
            waits = receive_m(s_m)
            next(waits)
            mf.start()
            next(waits, None)
            mn.start()

        for kind in table:
            gb, ga = kind.gb, kind.ga
            s_a3, s_swap, s_last = it - LAG_A[3], it - LAG_SWAP, it - LAG_X

            @pl.when(kind.has(s_a3))
            def _():
                kind.back_a(s_a3).wait_recv()
                j = s_a3 - kind.begin
                at = pl.multiple_of(kind.base + gb * kind.number + j * ga, 8)
                var_acc[pl.ds(at, ga), :] = square(kind.aq[j] + part[s_a3, kind.in_a])

            pl.when(kind.has(s_swap))(lambda: kind.swap(s_swap).start())

            @pl.when(kind.has(s_last))
            def _():
                kind.swap(s_last).wait_recv()
                j = s_last - kind.begin
                mine = pl.ds(pl.multiple_of(y * gb, 8), gb)
                at = pl.multiple_of(kind.base + j * gb, 8)
                var_acc[pl.ds(at, gb), :] = square(kind.bq[j, mine] + kind.got_x[j])

        means(it)
        return carry

    def middle_turn(it, carry):
        pl.when((it > 0) & (it < steps))(lambda: compute(it))
        send_y(it)
        for kind in table:
            s_1, s_2 = it - LAG_B[1], it - LAG_B[2]

            @pl.when(kind.has(s_1))
            def _():
                kind.first_b(s_1).wait_recv()
                j = s_1 - kind.begin
                kind.bp[j] = kind.bp[j] + part[s_1, kind.out_b]
                kind.cross_b(s_1).start()

            @pl.when(kind.has(s_2))
            def _():
                kind.cross_b(s_2).wait_recv()
                j = s_2 - kind.begin
                kind.bq[j] = kind.bq[j] + part[s_2, kind.in_b]
                kind.back_b(s_2).start()

        receive_y(it)
        s_m = it - LAG_M[0]

        @pl.when(m_has(s_m))
        def _():
            for _ in receive_m(s_m):
                pass

        for kind in table:
            s_1, s_2 = it - LAG_A[1], it - LAG_A[2]

            @pl.when(kind.has(s_1))
            def _():
                kind.first_a(s_1).wait_recv()
                j = s_1 - kind.begin
                kind.ap[j] = kind.ap[j] + part[s_1, kind.out_a]
                kind.cross_a(s_1).start()

            @pl.when(kind.has(s_2))
            def _():
                kind.cross_a(s_2).wait_recv()
                j = s_2 - kind.begin
                kind.aq[j] = kind.aq[j] + part[s_2, kind.in_a]
                kind.back_a(s_2).start()

        s_m1, s_m2 = it - LAG_M[1], it - LAG_M[2]

        @pl.when(m_has(s_m1))
        def _():
            m_first(s_m1)[0].wait_recv()
            j = s_m1 - m_begin
            got_mf[j] = got_mf[j] + part[s_m1, 2 * gm : 3 * gm]
            m_cross(s_m1).start()

        @pl.when(m_has(s_m2))
        def _():
            m_first(s_m2)[1].wait_recv()
            m_cross(s_m2).wait_recv()
            j = s_m2 - m_begin
            at = pl.multiple_of(m_base + j * gm, 8)
            var_acc[pl.ds(at, gm), :] = square(got_mn[j] + part[s_m2, 3 * gm :] + got_mx[j])

        means(it)
        return carry

    def settle_y():
        for kind in table:
            def done(s, carry):
                kind.copy_y(s).wait_send()
                return carry

            lax.fori_loop(kind.begin, kind.begin + kind.number, done, 0)

        for s in range(m_begin, m_begin + m_number):
            for copy in m_y(s):
                copy.wait_send()

    def collect(is_end):
        for k in range(1, LINE):
            mean_copy(k).wait()
        total = mean_box[0]
        for index in range(1, LINE):
            total = total + mean_box[index]
        out_ref[: rows // 128, :] = total
        settle_y()
        for kind in table:
            def done(s, carry):
                if is_end:
                    for copy in (kind.first_b(s), kind.first_a(s), kind.swap(s)):
                        copy.wait_send()
                else:
                    for copy in (kind.cross_b(s), kind.back_b(s), kind.cross_a(s), kind.back_a(s)):
                        copy.wait_send()
                return carry

            lax.fori_loop(kind.begin, kind.begin + kind.number, done, 0)
        for s in range(m_begin, m_begin + m_number):
            for copy in m_first(s) if is_end else (m_cross(s),):
                copy.wait_send()
        for who in range(4):
            if is_end:
                mid_copy(1, who).wait_recv()
                pl.when(owner != who)(lambda: var_copy(1, who).wait_recv())
            else:
                var_copy(1, who).wait_recv()
                pl.when(owner != who)(lambda: mid_copy(1, who).wait_recv())
        for who in range(4):
            begin = rows // 128 + who * lines
            out_ref[begin : begin + lines - 1, :] = 1.0 - var_box[who, : lines - 1]
            out_ref[begin + lines - 1 : begin + lines, :] = 1.0 - (var_box[who, lines - 1 :] + mid_box[who])
        for k in range(1, count):
            (var_copy if is_end else mid_copy)(k, owner).wait_send()

    compute(0, True)
    pl.semaphore_wait(barrier, count - 1)
    total_turns = steps + max(LAG_X, LAG_A[3], LAG_M[2])

    @pl.when(ends)
    def _():
        lax.fori_loop(0, total_turns, end_turn, 0)
        for index in range(lines):
            var_box[owner, index : index + 1, :] = line_of(index)
        for k in range(1, count):
            var_copy(k, owner).start()
        collect(True)

    @pl.when(jnp.logical_not(ends))
    def _():
        lax.fori_loop(0, total_turns, middle_turn, 0)
        mid_box[owner] = line_of(lines - 1)
        for k in range(1, count):
            mid_copy(k, owner).start()
        collect(False)


def fused(test_points, train_points, weights, factor, *, count):
    dim, rows = test_points.shape
    local = train_points.shape[1]
    width = factor.shape[1]
    depth = -(-(dim + 16) // 128) * 128
    steps = rows // BLOCK
    dma = pltpu.SemaphoreType.DMA
    f32 = jnp.float32
    kinds, (_, m_number, gm, _) = kinds_of(rows)
    sems = [dma((steps,))] * 12 + [dma((m_number,))] * 8
    sems += [dma((LINE,)), dma((LINE,)), dma((count,)), dma((4,)), dma((4,))]
    boxes = [pltpu.VMEM((m_number, gm, width), f32)] * 5
    for _, number, gb, ga, _ in kinds:
        for size in (2 * ga, 2 * gb, 2 * gb, ga, ga, gb):
            boxes.append(pltpu.VMEM((number, size, width), f32))
    out = pl.pallas_call(
        functools.partial(kernel, count=count),
        out_shape=pltpu.VMEM((rows // 64, 128), f32),
        in_specs=[pl.BlockSpec(memory_space=pl.ANY)] * 4,
        out_specs=pl.BlockSpec(memory_space=pltpu.VMEM),
        scratch_shapes=[
            pltpu.VMEM((dim, rows), jnp.bfloat16),
            pltpu.VMEM((local // 128, 128), jnp.bfloat16),
            pltpu.VMEM((local, width), jnp.bfloat16),
            dma((3 + local // CHUNK,)),
            pltpu.VMEM((rows, depth), f32),
            pltpu.VMEM((depth, local), jnp.bfloat16),
            pltpu.VMEM((1, local), f32),
            pltpu.VMEM((BLOCK, depth), jnp.bfloat16),
            pltpu.VMEM((steps, BLOCK, width), f32),
            pltpu.VMEM((rows, 128), f32),
            pltpu.VMEM((rows // 4, 128), f32),
            pltpu.VMEM((LINE + 1, rows // 128, 128), f32),
            pltpu.VMEM((4, rows // 512, 128), f32),
            pltpu.VMEM((4, 1, 128), f32),
        ] + sems + boxes,
        compiler_params=pltpu.CompilerParams(
            collective_id=0, has_side_effects=True, vmem_limit_bytes=40 * 1024 * 1024
        ),
    )(*[pltpu.with_memory_space_constraint(x, pltpu.HBM) for x in (test_points, train_points, weights.reshape(local // 128, 128), factor)])
    lines = rows // 128
    return out[:lines].reshape(rows), out[lines:].reshape(rows)


def on_device(test_points, train_points, weights, factor):
    rows = test_points.shape[1]
    local = train_points.shape[1]
    dim = test_points.shape[0]
    width = factor.shape[1]
    test_sq = jnp.sum(test_points.astype(jnp.float32) ** 2, axis=0)
    block = math.gcd(local, 1024)
    turns = local // block

    def step(index, carry):
        mean_acc, proj_acc = carry
        start = (index * block).astype(jnp.int32)
        points = lax.dynamic_slice_in_dim(train_points, start, block, 1)
        wblock = lax.dynamic_slice_in_dim(weights, start, block, 0)
        fblock = lax.dynamic_slice_in_dim(factor, start, block, 0)
        train_sq = jnp.sum(points.astype(jnp.float32) ** 2, axis=0)
        cross = lax.dot_general(
            test_points, points, (((0,), (0,)), ((), ())), preferred_element_type=jnp.float32
        )
        kernel = jnp.exp(
            -(test_sq[:, None] + train_sq[None, :] - 2.0 * cross) * (4.0 / dim)
        ).astype(jnp.bfloat16)
        mean_acc = mean_acc + jnp.dot(kernel, wblock, preferred_element_type=jnp.float32)
        proj_acc = proj_acc + jnp.dot(kernel, fblock, preferred_element_type=jnp.float32)
        return (mean_acc, proj_acc)

    init = (jnp.zeros((rows,), jnp.float32), jnp.zeros((rows, width), jnp.float32))
    mean_part, proj_part = lax.fori_loop(0, turns, step, init)
    mean_share, proj_share = (
        lax.psum_scatter(mean_part, "trn", scatter_dimension=0, tiled=True),
        lax.psum_scatter(proj_part, "trn", scatter_dimension=0, tiled=True),
    )
    var_share = 1.0 - jnp.sum(proj_share * proj_share, axis=1)
    mean, variance = (
        lax.all_gather(mean_share, "trn", axis=0, tiled=True),
        lax.all_gather(var_share, "trn", axis=0, tiled=True),
    )
    return (mean, variance)


def solution(mesh):
    in_specs = (
        P(None, ("grp", "tst")),
        P(None, ("grp", "trn")),
        P(("grp", "trn")),
        P(("grp", "trn"), None),
    )
    out_specs = (P(("grp", "tst")), P(("grp", "tst")))
    count = mesh.shape["trn"]
    body = functools.partial(fused, count=count) if count == 2 * LINE else on_device
    return jax.shard_map(
        body, mesh=mesh, in_specs=in_specs, out_specs=out_specs, check_vma=False
    )
```

```python
import functools
import math

import jax
import jax.numpy as jnp
from jax import lax
from jax.experimental import pallas as pl
from jax.experimental.pallas import tpu as pltpu
from jax.sharding import PartitionSpec as P

LOG2E = 1.4426950408889634
BLOCK = 128
CHUNK = 1024
LINE = 4
KINDS = ((10, 16, 16), (4, 8, 24))
MIDDLE = 2
LAG_Y = 3
LAG_B = (0, 2, 4, 11)
LAG_A = (3, 5, 8, 18)
LAG_SWAP = 11
LAG_X = 18
LAG_M = (4, 6, 17)
MEAN_AT = 1
MEAN_ON = 4


def pieces(value):
    high = value.astype(jnp.bfloat16).astype(jnp.float32)
    rest = value - high
    middle = rest.astype(jnp.bfloat16).astype(jnp.float32)
    low = (rest - middle).astype(jnp.bfloat16).astype(jnp.float32)
    return high, middle, low


def pick(row, table, default):
    value = default
    for index, entry in table:
        value = jnp.where(row == index, entry, value)
    return value


def kinds_of(rows):
    unit = rows // BLOCK // (MIDDLE + sum(count for count, _, _ in KINDS))
    table, begin, base = [], 0, 0
    for count, gb, ga in KINDS:
        count = count * unit
        table.append((begin, count, gb, ga, base))
        begin += count
        base += count * (gb + ga)
    return tuple(table), (begin, MIDDLE * unit, BLOCK // 4, base)


def kernel(
    test_hbm, train_hbm, weights_hbm, factor_hbm, out_ref,
    test_ref, weights_ref, factor_ref, in_sems,
    test_aug, train_aug, wide, left_ref, part, mean_acc, var_acc, mean_box, var_box, mid_box,
    s_y, r_y, s_b, rp_b, sq_b, rq_b, s_a, rp_a, sq_a, rq_a, s_x, r_x,
    s_yn, r_yn, s_mf, r_mf, s_mn, r_mn, s_mx, r_mx,
    s_mean, r_mean, s_var, r_var, r_mid, got_yf, got_yn, got_mf, got_mn, got_mx, *got, count,
):
    pair = count // LINE
    last = LINE - 1
    me = lax.axis_index("trn")
    z = me // pair
    y = me % pair
    dim, rows = test_ref.shape
    local = train_aug.shape[1]
    depth = test_aug.shape[1]
    steps = rows // BLOCK
    kinds, middle = kinds_of(rows)
    span = rows // 4
    other = z * pair + (1 - y)
    low = z < 2
    toward = jnp.where(low, me + pair, me - pair)
    back = jnp.where(low, me - pair, me + pair)
    far = jnp.where(low, 2, 0)
    near = 2 - far
    owner = near + y
    ends = (z == 0) | (z == last)
    chunks = local // CHUNK

    def fetch(index, source, target):
        return pltpu.make_async_copy(source, target, in_sems.at[index])

    fetch_train = fetch(0, train_hbm, train_aug.at[:dim])
    fetch_test = fetch(1, test_hbm, test_ref)
    fetch_weights = fetch(2, weights_hbm, weights_ref)

    def fetch_factor(index):
        block = pl.ds(index * CHUNK, CHUNK)
        return fetch(3 + index, factor_hbm.at[block], factor_ref.at[block])

    fetch_train.start()
    fetch_test.start()
    fetch_weights.start()
    for index in range(chunks):
        fetch_factor(index).start()

    barrier = pltpu.get_barrier_semaphore()
    for k in range(1, count):
        pl.semaphore_signal(barrier, inc=1, device_id={"trn": lax.rem(me + k, count)})

    var_acc[...] = jnp.zeros_like(var_acc)
    train_aug[dim + 16 :, :] = jnp.zeros((depth - dim - 16, local), jnp.bfloat16)
    fetch_train.wait()

    def prepare_train(index, carry):
        cols = pl.ds(pl.multiple_of(index * 512, 512), 512)
        points = train_aug[:dim, cols]
        squares = points.astype(jnp.float32) ** 2
        norm = jnp.sum(squares, axis=0, keepdims=True) * (-4.0 / dim)
        high, middle, low = pieces(norm)
        row = lax.broadcasted_iota(jnp.int32, (16, 512), 0)
        one = jnp.float32(1.0)
        extra = pick(row, ((0, one), (1, one), (2, one), (3, high), (4, middle), (5, low)), jnp.float32(0.0))
        train_aug[dim : dim + 16, cols] = extra.astype(jnp.bfloat16)
        return carry

    lax.fori_loop(0, local // 512, prepare_train, 0, unroll=True)
    fetch_test.wait()

    def prepare_test(index, carry):
        cols = pl.ds(pl.multiple_of(index * 256, 256), 256)
        points = test_ref[:, cols].astype(jnp.float32)
        norm = jnp.sum(points * points, axis=0, keepdims=True) * (-4.0 / dim)
        high, middle, low = pieces(norm)
        row = lax.broadcasted_iota(jnp.int32, (8, 256), 0)
        one = jnp.float32(1.0)
        extra = pick(row, ((0, high), (1, middle), (2, low), (3, one), (4, one), (5, one)), jnp.float32(0.0))
        whole = jnp.concatenate(
            [points * (8.0 / dim), extra, jnp.zeros((depth - dim - 8, 256), jnp.float32)], axis=0
        )
        test_aug[cols, :] = whole.T
        return carry

    lax.fori_loop(0, rows // 256, prepare_test, 0, unroll=True)
    fetch_weights.wait()
    for index in range(local // 128):
        wide[:, index * 128 : (index + 1) * 128] = weights_ref[index : index + 1, :].astype(jnp.float32)

    def edge_places(kind, step):
        begin, number, gb, ga, base = kind
        index = step - begin

        def row_of(who, early):
            inner = base + (number * gb + index * ga if early else index * gb)
            return pl.multiple_of(who * span + inner, 8)

        where = (
            row_of(far, False), row_of(far + 1, False), row_of(near, False), row_of(near + 1, False),
            row_of(far + 1 - y, True), row_of(near + 1 - y, True), row_of(far + y, True), row_of(near + y, True),
        )
        return tuple(zip(where, (gb,) * 4 + (ga,) * 4))

    def middle_places(step):
        begin, _, gm, base = middle
        inner = base + (step - begin) * gm
        who = (far + 1 - y, near + 1 - y, far + y, near + y)
        return tuple((pl.multiple_of(w * span + inner, 8), gm) for w in who)

    layouts = [(kind[0], kind[1], functools.partial(edge_places, kind)) for kind in kinds]
    layouts.append((middle[0], middle[1], middle_places))

    def compute(step, first=False):
        for begin, number, places in layouts:
            if first and begin > 0:
                continue

            def gather():
                left_ref[...] = jnp.concatenate(
                    [test_aug[pl.ds(at, size), :] for at, size in places(step)], axis=0
                ).astype(jnp.bfloat16)

            if first:
                gather()
            else:
                pl.when((step >= begin) & (step < begin + number))(gather)
        left = left_ref[...]
        total = None
        means = None
        held = []
        for index in range(chunks):
            begin = index * CHUNK
            power = jnp.dot(
                left, train_aug[:, begin : begin + CHUNK], preferred_element_type=jnp.float32
            )
            values = jnp.exp2(power * LOG2E).astype(jnp.bfloat16)
            scaled = values.astype(jnp.float32) * wide[:, begin : begin + CHUNK]
            for lane in range(0, CHUNK, 128):
                piece = scaled[:, lane : lane + 128]
                means = piece if means is None else means + piece
            if first:
                held.append(values)
                continue
            product = jnp.dot(
                values, factor_ref[begin : begin + CHUNK, :], preferred_element_type=jnp.float32
            )
            total = product if total is None else total + product
        if first:
            for index in range(chunks):
                fetch_factor(index).wait()
            total = jnp.dot(
                jnp.concatenate(held, axis=1), factor_ref[...], preferred_element_type=jnp.float32
            )
        part[step] = total
        mean_acc[pl.ds(pl.multiple_of(step * BLOCK, BLOCK), BLOCK), :] = means

    def send(source, target, ssem, rsem, device):
        return pltpu.make_async_remote_copy(
            src_ref=source, dst_ref=target, send_sem=ssem, recv_sem=rsem, device_id={"trn": device}
        )

    def square(values):
        total = None
        for lane in range(0, values.shape[1], 128):
            piece = values[:, lane : lane + 128]
            total = piece * piece if total is None else total + piece * piece
        return total

    class Kind:
        def __init__(self, kind, buffers):
            self.begin, self.number, self.gb, self.ga, self.base = kind
            self.got_y, self.bp, self.bq, self.ap, self.aq, self.got_x = buffers
            gb, ga = self.gb, self.ga
            self.sent = slice(4 * gb, 4 * gb + 2 * ga)
            self.kept = slice(4 * gb + 2 * ga, 4 * gb + 4 * ga)
            self.out_b, self.in_b = slice(0, 2 * gb), slice(2 * gb, 4 * gb)
            self.out_a = slice(4 * gb + 2 * ga, 4 * gb + 3 * ga)
            self.in_a = slice(4 * gb + 3 * ga, 4 * gb + 4 * ga)

        def has(self, s):
            return (s >= self.begin) & (s < self.begin + self.number)

        def copy_y(self, s):
            return send(part.at[s, self.sent], self.got_y.at[s - self.begin], s_y.at[s], r_y.at[s], other)

        def first_b(self, s):
            return send(part.at[s, self.out_b], self.bp.at[s - self.begin], s_b.at[s], rp_b.at[s], toward)

        def cross_b(self, s):
            j = s - self.begin
            return send(self.bp.at[j], self.bq.at[j], s_b.at[s], rq_b.at[s], toward)

        def back_b(self, s):
            j = s - self.begin
            return send(self.bq.at[j], self.bq.at[j], sq_b.at[s], rq_b.at[s], back)

        def first_a(self, s):
            return send(part.at[s, self.out_a], self.ap.at[s - self.begin], s_a.at[s], rp_a.at[s], toward)

        def cross_a(self, s):
            j = s - self.begin
            return send(self.ap.at[j], self.aq.at[j], s_a.at[s], rq_a.at[s], toward)

        def back_a(self, s):
            j = s - self.begin
            return send(self.aq.at[j], self.aq.at[j], sq_a.at[s], rq_a.at[s], back)

        def swap(self, s):
            j = s - self.begin
            theirs = pl.ds(pl.multiple_of((1 - y) * self.gb, 8), self.gb)
            return send(self.bq.at[j, theirs], self.got_x.at[j], s_x.at[s], r_x.at[s], other)

    table = [Kind(kind, got[6 * i : 6 * i + 6]) for i, kind in enumerate(kinds)]
    m_begin, m_number, gm, m_base = middle

    def m_has(s):
        return (s >= m_begin) & (s < m_begin + m_number)

    def m_y(s):
        j = s - m_begin
        return (
            send(part.at[s, :gm], got_yf.at[j], s_y.at[s], r_y.at[s], other),
            send(part.at[s, gm : 2 * gm], got_yn.at[j], s_yn.at[j], r_yn.at[j], other),
        )

    def m_first(s):
        j = s - m_begin
        return (
            send(part.at[s, 2 * gm : 3 * gm], got_mf.at[j], s_mf.at[j], r_mf.at[j], toward),
            send(part.at[s, 3 * gm :], got_mn.at[j], s_mn.at[j], r_mn.at[j], toward),
        )

    def m_cross(s):
        j = s - m_begin
        return send(got_mf.at[j], got_mx.at[j], s_mx.at[j], r_mx.at[j], toward)

    def mean_swap():
        return send(mean_box.at[z], mean_box.at[LINE], s_mean.at[0], r_mean.at[0], other)

    def mean_copy(k):
        target = lax.rem(me + k * pair, count)
        return send(mean_box.at[z], mean_box.at[z], s_mean.at[k], r_mean.at[k], target)

    def mean_start():
        for begin, number, places in layouts:
            def place(step, carry):
                start = pl.multiple_of(step * BLOCK, BLOCK)
                for at, size in places(step):
                    test_aug[pl.ds(at, size), :] = mean_acc[pl.ds(start, size), :]
                    start = pl.multiple_of(start + size, 8)
                return carry

            lax.fori_loop(begin, begin + number, place, 0)
        for index in range(rows // 128):
            block = test_aug[index * 128 : (index + 1) * 128, :]
            mean_box[z, index : index + 1, :] = jnp.sum(block.T, axis=0, keepdims=True)
        mean_swap().start()

    def mean_spread():
        mean_swap().wait()
        mean_box[z] = mean_box[z] + mean_box[LINE]
        for k in range(1, LINE):
            mean_copy(k).start()

    lines = span // 128

    def line_of(index):
        block = var_acc[index * 128 : (index + 1) * 128, :]
        return jnp.sum(block.T, axis=0, keepdims=True)

    def var_copy(k, who):
        return send(var_box.at[who], var_box.at[who], s_var.at[k], r_var.at[who], lax.rem(me + k, count))

    def mid_copy(k, who):
        return send(mid_box.at[who], mid_box.at[who], s_var.at[k], r_mid.at[who], lax.rem(me + k, count))

    def receive_y(it):
        for kind in table:
            s = it - LAG_Y

            @pl.when(kind.has(s))
            def _():
                kind.copy_y(s).wait_recv()
                part[s, kind.kept] = part[s, kind.kept] + kind.got_y[s - kind.begin]

    def receive_m(s):
        j = s - m_begin
        yf, yn = m_y(s)
        yf.wait_recv()
        part[s, 2 * gm : 3 * gm] = part[s, 2 * gm : 3 * gm] + got_yf[j]
        yield
        yn.wait_recv()
        part[s, 3 * gm :] = part[s, 3 * gm :] + got_yn[j]

    def send_y(it):
        for kind in table:
            pl.when(kind.has(it))(lambda: kind.copy_y(it).start())

        @pl.when(m_has(it))
        def _():
            for copy in m_y(it):
                copy.start()

    def means(it):
        pl.when(it == steps + MEAN_AT)(mean_start)
        pl.when(it == steps + MEAN_ON)(mean_spread)

    def end_turn(it, carry):
        pl.when((it > 0) & (it < steps))(lambda: compute(it))
        for kind in table:
            pl.when(kind.has(it))(lambda: kind.first_b(it).start())
        send_y(it)
        receive_y(it)
        for kind in table:
            s_go = it - LAG_A[0]
            pl.when(kind.has(s_go))(lambda: kind.first_a(s_go).start())
        for kind in table:
            s_hold = it - LAG_B[3]

            @pl.when(kind.has(s_hold))
            def _():
                kind.back_b(s_hold).wait_recv()
                j = s_hold - kind.begin
                kind.bq[j] = kind.bq[j] + part[s_hold, kind.in_b]

        s_m = it - LAG_M[0]

        @pl.when(m_has(s_m))
        def _():
            mf, mn = m_first(s_m)
            waits = receive_m(s_m)
            next(waits)
            mf.start()
            next(waits, None)
            mn.start()

        for kind in table:
            gb, ga = kind.gb, kind.ga
            s_a3, s_swap, s_last = it - LAG_A[3], it - LAG_SWAP, it - LAG_X

            @pl.when(kind.has(s_a3))
            def _():
                kind.back_a(s_a3).wait_recv()
                j = s_a3 - kind.begin
                at = pl.multiple_of(kind.base + gb * kind.number + j * ga, 8)
                var_acc[pl.ds(at, ga), :] = square(kind.aq[j] + part[s_a3, kind.in_a])

            pl.when(kind.has(s_swap))(lambda: kind.swap(s_swap).start())

            @pl.when(kind.has(s_last))
            def _():
                kind.swap(s_last).wait_recv()
                j = s_last - kind.begin
                mine = pl.ds(pl.multiple_of(y * gb, 8), gb)
                at = pl.multiple_of(kind.base + j * gb, 8)
                var_acc[pl.ds(at, gb), :] = square(kind.bq[j, mine] + kind.got_x[j])

        means(it)
        return carry

    def middle_turn(it, carry):
        pl.when((it > 0) & (it < steps))(lambda: compute(it))
        send_y(it)
        for kind in table:
            s_1, s_2 = it - LAG_B[1], it - LAG_B[2]

            @pl.when(kind.has(s_1))
            def _():
                kind.first_b(s_1).wait_recv()
                j = s_1 - kind.begin
                kind.bp[j] = kind.bp[j] + part[s_1, kind.out_b]
                kind.cross_b(s_1).start()

            @pl.when(kind.has(s_2))
            def _():
                kind.cross_b(s_2).wait_recv()
                j = s_2 - kind.begin
                kind.bq[j] = kind.bq[j] + part[s_2, kind.in_b]
                kind.back_b(s_2).start()

        receive_y(it)
        s_m = it - LAG_M[0]

        @pl.when(m_has(s_m))
        def _():
            for _ in receive_m(s_m):
                pass

        for kind in table:
            s_1, s_2 = it - LAG_A[1], it - LAG_A[2]

            @pl.when(kind.has(s_1))
            def _():
                kind.first_a(s_1).wait_recv()
                j = s_1 - kind.begin
                kind.ap[j] = kind.ap[j] + part[s_1, kind.out_a]
                kind.cross_a(s_1).start()

            @pl.when(kind.has(s_2))
            def _():
                kind.cross_a(s_2).wait_recv()
                j = s_2 - kind.begin
                kind.aq[j] = kind.aq[j] + part[s_2, kind.in_a]
                kind.back_a(s_2).start()

        s_m1, s_m2 = it - LAG_M[1], it - LAG_M[2]

        @pl.when(m_has(s_m1))
        def _():
            m_first(s_m1)[0].wait_recv()
            j = s_m1 - m_begin
            got_mf[j] = got_mf[j] + part[s_m1, 2 * gm : 3 * gm]
            m_cross(s_m1).start()

        @pl.when(m_has(s_m2))
        def _():
            m_first(s_m2)[1].wait_recv()
            m_cross(s_m2).wait_recv()
            j = s_m2 - m_begin
            at = pl.multiple_of(m_base + j * gm, 8)
            var_acc[pl.ds(at, gm), :] = square(got_mn[j] + part[s_m2, 3 * gm :] + got_mx[j])

        means(it)
        return carry

    def settle_y():
        for kind in table:
            def done(s, carry):
                kind.copy_y(s).wait_send()
                return carry

            lax.fori_loop(kind.begin, kind.begin + kind.number, done, 0)

        for s in range(m_begin, m_begin + m_number):
            for copy in m_y(s):
                copy.wait_send()

    def collect(is_end):
        for k in range(1, LINE):
            mean_copy(k).wait()
        total = mean_box[0]
        for index in range(1, LINE):
            total = total + mean_box[index]
        out_ref[: rows // 128, :] = total
        settle_y()
        for kind in table:
            def done(s, carry):
                if is_end:
                    for copy in (kind.first_b(s), kind.first_a(s), kind.swap(s)):
                        copy.wait_send()
                else:
                    for copy in (kind.cross_b(s), kind.back_b(s), kind.cross_a(s), kind.back_a(s)):
                        copy.wait_send()
                return carry

            lax.fori_loop(kind.begin, kind.begin + kind.number, done, 0)
        for s in range(m_begin, m_begin + m_number):
            for copy in m_first(s) if is_end else (m_cross(s),):
                copy.wait_send()
        for who in range(4):
            if is_end:
                mid_copy(1, who).wait_recv()
                pl.when(owner != who)(lambda: var_copy(1, who).wait_recv())
            else:
                var_copy(1, who).wait_recv()
                pl.when(owner != who)(lambda: mid_copy(1, who).wait_recv())
        for who in range(4):
            begin = rows // 128 + who * lines
            out_ref[begin : begin + lines - 1, :] = 1.0 - var_box[who, : lines - 1]
            out_ref[begin + lines - 1 : begin + lines, :] = 1.0 - (var_box[who, lines - 1 :] + mid_box[who])
        for k in range(1, count):
            (var_copy if is_end else mid_copy)(k, owner).wait_send()

    compute(0, True)
    pl.semaphore_wait(barrier, count - 1)
    total_turns = steps + max(LAG_X, LAG_A[3], LAG_M[2])

    @pl.when(ends)
    def _():
        lax.fori_loop(0, total_turns, end_turn, 0)
        for index in range(lines):
            var_box[owner, index : index + 1, :] = line_of(index)
        for k in range(1, count):
            var_copy(k, owner).start()
        collect(True)

    @pl.when(jnp.logical_not(ends))
    def _():
        lax.fori_loop(0, total_turns, middle_turn, 0)
        mid_box[owner] = line_of(lines - 1)
        for k in range(1, count):
            mid_copy(k, owner).start()
        collect(False)


def fused(test_points, train_points, weights, factor, *, count):
    dim, rows = test_points.shape
    local = train_points.shape[1]
    width = factor.shape[1]
    depth = -(-(dim + 16) // 128) * 128
    steps = rows // BLOCK
    dma = pltpu.SemaphoreType.DMA
    f32 = jnp.float32
    kinds, (_, m_number, gm, _) = kinds_of(rows)
    sems = [dma((steps,))] * 12 + [dma((m_number,))] * 8
    sems += [dma((LINE,)), dma((LINE,)), dma((count,)), dma((4,)), dma((4,))]
    boxes = [pltpu.VMEM((m_number, gm, width), f32)] * 5
    for _, number, gb, ga, _ in kinds:
        for size in (2 * ga, 2 * gb, 2 * gb, ga, ga, gb):
            boxes.append(pltpu.VMEM((number, size, width), f32))
    out = pl.pallas_call(
        functools.partial(kernel, count=count),
        out_shape=pltpu.VMEM((rows // 64, 128), f32),
        in_specs=[pl.BlockSpec(memory_space=pl.ANY)] * 4,
        out_specs=pl.BlockSpec(memory_space=pltpu.VMEM),
        scratch_shapes=[
            pltpu.VMEM((dim, rows), jnp.bfloat16),
            pltpu.VMEM((local // 128, 128), jnp.bfloat16),
            pltpu.VMEM((local, width), jnp.bfloat16),
            dma((3 + local // CHUNK,)),
            pltpu.VMEM((rows, depth), f32),
            pltpu.VMEM((depth, local), jnp.bfloat16),
            pltpu.VMEM((1, local), f32),
            pltpu.VMEM((BLOCK, depth), jnp.bfloat16),
            pltpu.VMEM((steps, BLOCK, width), f32),
            pltpu.VMEM((rows, 128), f32),
            pltpu.VMEM((rows // 4, 128), f32),
            pltpu.VMEM((LINE + 1, rows // 128, 128), f32),
            pltpu.VMEM((4, rows // 512, 128), f32),
            pltpu.VMEM((4, 1, 128), f32),
        ] + sems + boxes,
        compiler_params=pltpu.CompilerParams(
            collective_id=0, has_side_effects=True, vmem_limit_bytes=40 * 1024 * 1024
        ),
    )(*[pltpu.with_memory_space_constraint(x, pltpu.HBM) for x in (test_points, train_points, weights.reshape(local // 128, 128), factor)])
    lines = rows // 128
    return out[:lines].reshape(rows), out[lines:].reshape(rows)


def on_device(test_points, train_points, weights, factor):
    rows = test_points.shape[1]
    local = train_points.shape[1]
    dim = test_points.shape[0]
    width = factor.shape[1]
    test_sq = jnp.sum(test_points.astype(jnp.float32) ** 2, axis=0)
    block = math.gcd(local, 1024)
    turns = local // block

    def step(index, carry):
        mean_acc, proj_acc = carry
        start = (index * block).astype(jnp.int32)
        points = lax.dynamic_slice_in_dim(train_points, start, block, 1)
        wblock = lax.dynamic_slice_in_dim(weights, start, block, 0)
        fblock = lax.dynamic_slice_in_dim(factor, start, block, 0)
        train_sq = jnp.sum(points.astype(jnp.float32) ** 2, axis=0)
        cross = lax.dot_general(
            test_points, points, (((0,), (0,)), ((), ())), preferred_element_type=jnp.float32
        )
        kernel = jnp.exp(
            -(test_sq[:, None] + train_sq[None, :] - 2.0 * cross) * (4.0 / dim)
        ).astype(jnp.bfloat16)
        mean_acc = mean_acc + jnp.dot(kernel, wblock, preferred_element_type=jnp.float32)
        proj_acc = proj_acc + jnp.dot(kernel, fblock, preferred_element_type=jnp.float32)
        return (mean_acc, proj_acc)

    init = (jnp.zeros((rows,), jnp.float32), jnp.zeros((rows, width), jnp.float32))
    mean_part, proj_part = lax.fori_loop(0, turns, step, init)
    mean_share, proj_share = (
        lax.psum_scatter(mean_part, "trn", scatter_dimension=0, tiled=True),
        lax.psum_scatter(proj_part, "trn", scatter_dimension=0, tiled=True),
    )
    var_share = 1.0 - jnp.sum(proj_share * proj_share, axis=1)
    mean, variance = (
        lax.all_gather(mean_share, "trn", axis=0, tiled=True),
        lax.all_gather(var_share, "trn", axis=0, tiled=True),
    )
    return (mean, variance)


def solution(mesh):
    in_specs = (
        P(None, ("grp", "tst")),
        P(None, ("grp", "trn")),
        P(("grp", "trn")),
        P(("grp", "trn"), None),
    )
    out_specs = (P(("grp", "tst")), P(("grp", "tst")))
    count = mesh.shape["trn"]
    body = functools.partial(fused, count=count) if count == 2 * LINE else on_device
    return jax.shard_map(
        body, mesh=mesh, in_specs=in_specs, out_specs=out_specs, check_vma=False
    )
```

```python
import functools
import math

import jax
import jax.numpy as jnp
from jax import lax
from jax.experimental import pallas as pl
from jax.experimental.pallas import tpu as pltpu
from jax.sharding import PartitionSpec as P

LOG2E = 1.4426950408889634
BLOCK = 128
CHUNK = 1024
LINE = 4
KINDS = ((10, 16, 16), (4, 8, 24))
MIDDLE = 2
LAG_Y = 3
LAG_B = (0, 2, 4, 11)
LAG_A = (3, 5, 8, 18)
LAG_SWAP = 11
LAG_X = 18
LAG_M = (4, 6, 14)
MEAN_AT = 1
MEAN_ON = 4


def pieces(value):
    high = value.astype(jnp.bfloat16).astype(jnp.float32)
    rest = value - high
    middle = rest.astype(jnp.bfloat16).astype(jnp.float32)
    low = (rest - middle).astype(jnp.bfloat16).astype(jnp.float32)
    return high, middle, low


def pick(row, table, default):
    value = default
    for index, entry in table:
        value = jnp.where(row == index, entry, value)
    return value


def kinds_of(rows):
    unit = rows // BLOCK // (MIDDLE + sum(count for count, _, _ in KINDS))
    table, begin, base = [], 0, 0
    for count, gb, ga in KINDS:
        count = count * unit
        table.append((begin, count, gb, ga, base))
        begin += count
        base += count * (gb + ga)
    return tuple(table), (begin, MIDDLE * unit, BLOCK // 4, base)


def kernel(
    test_hbm, train_hbm, weights_hbm, factor_hbm, out_ref,
    test_ref, weights_ref, factor_ref, in_sems,
    test_aug, train_aug, wide, left_ref, part, mean_acc, var_acc, mean_box, var_box, mid_box,
    s_y, r_y, s_b, rp_b, sq_b, rq_b, s_a, rp_a, sq_a, rq_a, s_x, r_x,
    s_yn, r_yn, s_mf, r_mf, s_mn, r_mn, s_mx, r_mx,
    s_mean, r_mean, s_var, r_var, r_mid, got_yf, got_yn, got_mf, got_mn, got_mx, *got, count,
):
    pair = count // LINE
    last = LINE - 1
    me = lax.axis_index("trn")
    z = me // pair
    y = me % pair
    dim, rows = test_ref.shape
    local = train_aug.shape[1]
    depth = test_aug.shape[1]
    steps = rows // BLOCK
    kinds, middle = kinds_of(rows)
    span = rows // 4
    other = z * pair + (1 - y)
    low = z < 2
    toward = jnp.where(low, me + pair, me - pair)
    back = jnp.where(low, me - pair, me + pair)
    far = jnp.where(low, 2, 0)
    near = 2 - far
    owner = near + y
    ends = (z == 0) | (z == last)
    chunks = local // CHUNK

    def fetch(index, source, target):
        return pltpu.make_async_copy(source, target, in_sems.at[index])

    fetch_train = fetch(0, train_hbm, train_aug.at[:dim])
    fetch_test = fetch(1, test_hbm, test_ref)
    fetch_weights = fetch(2, weights_hbm, weights_ref)

    def fetch_factor(index):
        block = pl.ds(index * CHUNK, CHUNK)
        return fetch(3 + index, factor_hbm.at[block], factor_ref.at[block])

    fetch_train.start()
    fetch_test.start()
    fetch_weights.start()
    for index in range(chunks):
        fetch_factor(index).start()

    barrier = pltpu.get_barrier_semaphore()
    for k in range(1, count):
        pl.semaphore_signal(barrier, inc=1, device_id={"trn": lax.rem(me + k, count)})

    var_acc[...] = jnp.zeros_like(var_acc)
    train_aug[dim + 16 :, :] = jnp.zeros((depth - dim - 16, local), jnp.bfloat16)
    fetch_train.wait()

    def prepare_train(index, carry):
        cols = pl.ds(pl.multiple_of(index * 512, 512), 512)
        points = train_aug[:dim, cols]
        squares = points.astype(jnp.float32) ** 2
        norm = jnp.sum(squares, axis=0, keepdims=True) * (-4.0 / dim)
        high, middle, low = pieces(norm)
        row = lax.broadcasted_iota(jnp.int32, (16, 512), 0)
        one = jnp.float32(1.0)
        extra = pick(row, ((0, one), (1, one), (2, one), (3, high), (4, middle), (5, low)), jnp.float32(0.0))
        train_aug[dim : dim + 16, cols] = extra.astype(jnp.bfloat16)
        return carry

    lax.fori_loop(0, local // 512, prepare_train, 0, unroll=True)
    fetch_test.wait()

    def prepare_test(index, carry):
        cols = pl.ds(pl.multiple_of(index * 256, 256), 256)
        points = test_ref[:, cols].astype(jnp.float32)
        norm = jnp.sum(points * points, axis=0, keepdims=True) * (-4.0 / dim)
        high, middle, low = pieces(norm)
        row = lax.broadcasted_iota(jnp.int32, (8, 256), 0)
        one = jnp.float32(1.0)
        extra = pick(row, ((0, high), (1, middle), (2, low), (3, one), (4, one), (5, one)), jnp.float32(0.0))
        whole = jnp.concatenate(
            [points * (8.0 / dim), extra, jnp.zeros((depth - dim - 8, 256), jnp.float32)], axis=0
        )
        test_aug[cols, :] = whole.T
        return carry

    lax.fori_loop(0, rows // 256, prepare_test, 0, unroll=True)
    fetch_weights.wait()
    for index in range(local // 128):
        wide[:, index * 128 : (index + 1) * 128] = weights_ref[index : index + 1, :].astype(jnp.float32)

    def edge_places(kind, step):
        begin, number, gb, ga, base = kind
        index = step - begin

        def row_of(who, early):
            inner = base + (number * gb + index * ga if early else index * gb)
            return pl.multiple_of(who * span + inner, 8)

        where = (
            row_of(far, False), row_of(far + 1, False), row_of(near, False), row_of(near + 1, False),
            row_of(far + 1 - y, True), row_of(near + 1 - y, True), row_of(far + y, True), row_of(near + y, True),
        )
        return tuple(zip(where, (gb,) * 4 + (ga,) * 4))

    def middle_places(step):
        begin, _, gm, base = middle
        inner = base + (step - begin) * gm
        who = (far + 1 - y, near + 1 - y, far + y, near + y)
        return tuple((pl.multiple_of(w * span + inner, 8), gm) for w in who)

    layouts = [(kind[0], kind[1], functools.partial(edge_places, kind)) for kind in kinds]
    layouts.append((middle[0], middle[1], middle_places))

    def compute(step, first=False):
        for begin, number, places in layouts:
            if first and begin > 0:
                continue

            def gather():
                left_ref[...] = jnp.concatenate(
                    [test_aug[pl.ds(at, size), :] for at, size in places(step)], axis=0
                ).astype(jnp.bfloat16)

            if first:
                gather()
            else:
                pl.when((step >= begin) & (step < begin + number))(gather)
        left = left_ref[...]
        total = None
        means = None
        held = []
        for index in range(chunks):
            begin = index * CHUNK
            power = jnp.dot(
                left, train_aug[:, begin : begin + CHUNK], preferred_element_type=jnp.float32
            )
            values = jnp.exp2(power * LOG2E).astype(jnp.bfloat16)
            scaled = values.astype(jnp.float32) * wide[:, begin : begin + CHUNK]
            for lane in range(0, CHUNK, 128):
                piece = scaled[:, lane : lane + 128]
                means = piece if means is None else means + piece
            if first:
                held.append(values)
                continue
            product = jnp.dot(
                values, factor_ref[begin : begin + CHUNK, :], preferred_element_type=jnp.float32
            )
            total = product if total is None else total + product
        if first:
            for index in range(chunks):
                fetch_factor(index).wait()
            total = jnp.dot(
                jnp.concatenate(held, axis=1), factor_ref[...], preferred_element_type=jnp.float32
            )
        part[step] = total
        mean_acc[pl.ds(pl.multiple_of(step * BLOCK, BLOCK), BLOCK), :] = means

    def send(source, target, ssem, rsem, device):
        return pltpu.make_async_remote_copy(
            src_ref=source, dst_ref=target, send_sem=ssem, recv_sem=rsem, device_id={"trn": device}
        )

    def square(values):
        total = None
        for lane in range(0, values.shape[1], 128):
            piece = values[:, lane : lane + 128]
            total = piece * piece if total is None else total + piece * piece
        return total

    class Kind:
        def __init__(self, kind, buffers):
            self.begin, self.number, self.gb, self.ga, self.base = kind
            self.got_y, self.bp, self.bq, self.ap, self.aq, self.got_x = buffers
            gb, ga = self.gb, self.ga
            self.sent = slice(4 * gb, 4 * gb + 2 * ga)
            self.kept = slice(4 * gb + 2 * ga, 4 * gb + 4 * ga)
            self.out_b, self.in_b = slice(0, 2 * gb), slice(2 * gb, 4 * gb)
            self.out_a = slice(4 * gb + 2 * ga, 4 * gb + 3 * ga)
            self.in_a = slice(4 * gb + 3 * ga, 4 * gb + 4 * ga)

        def has(self, s):
            return (s >= self.begin) & (s < self.begin + self.number)

        def copy_y(self, s):
            return send(part.at[s, self.sent], self.got_y.at[s - self.begin], s_y.at[s], r_y.at[s], other)

        def first_b(self, s):
            return send(part.at[s, self.out_b], self.bp.at[s - self.begin], s_b.at[s], rp_b.at[s], toward)

        def cross_b(self, s):
            j = s - self.begin
            return send(self.bp.at[j], self.bq.at[j], s_b.at[s], rq_b.at[s], toward)

        def back_b(self, s):
            j = s - self.begin
            return send(self.bq.at[j], self.bq.at[j], sq_b.at[s], rq_b.at[s], back)

        def first_a(self, s):
            return send(part.at[s, self.out_a], self.ap.at[s - self.begin], s_a.at[s], rp_a.at[s], toward)

        def cross_a(self, s):
            j = s - self.begin
            return send(self.ap.at[j], self.aq.at[j], s_a.at[s], rq_a.at[s], toward)

        def back_a(self, s):
            j = s - self.begin
            return send(self.aq.at[j], self.aq.at[j], sq_a.at[s], rq_a.at[s], back)

        def swap(self, s):
            j = s - self.begin
            theirs = pl.ds(pl.multiple_of((1 - y) * self.gb, 8), self.gb)
            return send(self.bq.at[j, theirs], self.got_x.at[j], s_x.at[s], r_x.at[s], other)

    table = [Kind(kind, got[6 * i : 6 * i + 6]) for i, kind in enumerate(kinds)]
    m_begin, m_number, gm, m_base = middle

    def m_has(s):
        return (s >= m_begin) & (s < m_begin + m_number)

    def m_y(s):
        j = s - m_begin
        return (
            send(part.at[s, :gm], got_yf.at[j], s_y.at[s], r_y.at[s], other),
            send(part.at[s, gm : 2 * gm], got_yn.at[j], s_yn.at[j], r_yn.at[j], other),
        )

    def m_first(s):
        j = s - m_begin
        return (
            send(part.at[s, 2 * gm : 3 * gm], got_mf.at[j], s_mf.at[j], r_mf.at[j], toward),
            send(part.at[s, 3 * gm :], got_mn.at[j], s_mn.at[j], r_mn.at[j], toward),
        )

    def m_cross(s):
        j = s - m_begin
        return send(got_mf.at[j], got_mx.at[j], s_mx.at[j], r_mx.at[j], toward)

    def mean_swap():
        return send(mean_box.at[z], mean_box.at[LINE], s_mean.at[0], r_mean.at[0], other)

    def mean_copy(k):
        target = lax.rem(me + k * pair, count)
        return send(mean_box.at[z], mean_box.at[z], s_mean.at[k], r_mean.at[k], target)

    def mean_start():
        for begin, number, places in layouts:
            def place(step, carry):
                start = pl.multiple_of(step * BLOCK, BLOCK)
                for at, size in places(step):
                    test_aug[pl.ds(at, size), :] = mean_acc[pl.ds(start, size), :]
                    start = pl.multiple_of(start + size, 8)
                return carry

            lax.fori_loop(begin, begin + number, place, 0)
        for index in range(rows // 128):
            block = test_aug[index * 128 : (index + 1) * 128, :]
            mean_box[z, index : index + 1, :] = jnp.sum(block.T, axis=0, keepdims=True)
        mean_swap().start()

    def mean_spread():
        mean_swap().wait()
        mean_box[z] = mean_box[z] + mean_box[LINE]
        for k in range(1, LINE):
            mean_copy(k).start()

    lines = span // 128

    def line_of(index):
        block = var_acc[index * 128 : (index + 1) * 128, :]
        return jnp.sum(block.T, axis=0, keepdims=True)

    def var_copy(k, who):
        return send(var_box.at[who], var_box.at[who], s_var.at[k], r_var.at[who], lax.rem(me + k, count))

    def mid_copy(k, who):
        return send(mid_box.at[who], mid_box.at[who], s_var.at[k], r_mid.at[who], lax.rem(me + k, count))

    def receive_y(it):
        for kind in table:
            s = it - LAG_Y

            @pl.when(kind.has(s))
            def _():
                kind.copy_y(s).wait_recv()
                part[s, kind.kept] = part[s, kind.kept] + kind.got_y[s - kind.begin]

    def receive_m(s):
        j = s - m_begin
        yf, yn = m_y(s)
        yf.wait_recv()
        part[s, 2 * gm : 3 * gm] = part[s, 2 * gm : 3 * gm] + got_yf[j]
        yield
        yn.wait_recv()
        part[s, 3 * gm :] = part[s, 3 * gm :] + got_yn[j]

    def send_y(it):
        for kind in table:
            pl.when(kind.has(it))(lambda: kind.copy_y(it).start())

        @pl.when(m_has(it))
        def _():
            for copy in m_y(it):
                copy.start()

    def means(it):
        pl.when(it == steps + MEAN_AT)(mean_start)
        pl.when(it == steps + MEAN_ON)(mean_spread)

    def end_turn(it, carry):
        pl.when((it > 0) & (it < steps))(lambda: compute(it))
        for kind in table:
            pl.when(kind.has(it))(lambda: kind.first_b(it).start())
        send_y(it)
        for kind in table:
            s_hold = it - LAG_B[3]

            @pl.when(kind.has(s_hold))
            def _():
                kind.back_b(s_hold).wait_recv()
                j = s_hold - kind.begin
                kind.bq[j] = kind.bq[j] + part[s_hold, kind.in_b]

        receive_y(it)
        for kind in table:
            s_go = it - LAG_A[0]
            pl.when(kind.has(s_go))(lambda: kind.first_a(s_go).start())
        s_m = it - LAG_M[0]

        @pl.when(m_has(s_m))
        def _():
            mf, mn = m_first(s_m)
            waits = receive_m(s_m)
            next(waits)
            mf.start()
            next(waits, None)
            mn.start()

        for kind in table:
            gb, ga = kind.gb, kind.ga
            s_a3, s_swap, s_last = it - LAG_A[3], it - LAG_SWAP, it - LAG_X

            @pl.when(kind.has(s_a3))
            def _():
                kind.back_a(s_a3).wait_recv()
                j = s_a3 - kind.begin
                at = pl.multiple_of(kind.base + gb * kind.number + j * ga, 8)
                var_acc[pl.ds(at, ga), :] = square(kind.aq[j] + part[s_a3, kind.in_a])

            pl.when(kind.has(s_swap))(lambda: kind.swap(s_swap).start())

            @pl.when(kind.has(s_last))
            def _():
                kind.swap(s_last).wait_recv()
                j = s_last - kind.begin
                mine = pl.ds(pl.multiple_of(y * gb, 8), gb)
                at = pl.multiple_of(kind.base + j * gb, 8)
                var_acc[pl.ds(at, gb), :] = square(kind.bq[j, mine] + kind.got_x[j])

        means(it)
        return carry

    def middle_turn(it, carry):
        pl.when((it > 0) & (it < steps))(lambda: compute(it))
        send_y(it)
        for kind in table:
            s_1, s_2 = it - LAG_B[1], it - LAG_B[2]

            @pl.when(kind.has(s_1))
            def _():
                kind.first_b(s_1).wait_recv()
                j = s_1 - kind.begin
                kind.bp[j] = kind.bp[j] + part[s_1, kind.out_b]
                kind.cross_b(s_1).start()

            @pl.when(kind.has(s_2))
            def _():
                kind.cross_b(s_2).wait_recv()
                j = s_2 - kind.begin
                kind.bq[j] = kind.bq[j] + part[s_2, kind.in_b]
                kind.back_b(s_2).start()

        receive_y(it)
        s_m = it - LAG_M[0]

        @pl.when(m_has(s_m))
        def _():
            for _ in receive_m(s_m):
                pass

        for kind in table:
            s_1, s_2 = it - LAG_A[1], it - LAG_A[2]

            @pl.when(kind.has(s_1))
            def _():
                kind.first_a(s_1).wait_recv()
                j = s_1 - kind.begin
                kind.ap[j] = kind.ap[j] + part[s_1, kind.out_a]
                kind.cross_a(s_1).start()

            @pl.when(kind.has(s_2))
            def _():
                kind.cross_a(s_2).wait_recv()
                j = s_2 - kind.begin
                kind.aq[j] = kind.aq[j] + part[s_2, kind.in_a]
                kind.back_a(s_2).start()

        s_m1, s_m2 = it - LAG_M[1], it - LAG_M[2]

        @pl.when(m_has(s_m1))
        def _():
            m_first(s_m1)[0].wait_recv()
            j = s_m1 - m_begin
            got_mf[j] = got_mf[j] + part[s_m1, 2 * gm : 3 * gm]
            m_cross(s_m1).start()

        @pl.when(m_has(s_m2))
        def _():
            m_first(s_m2)[1].wait_recv()
            m_cross(s_m2).wait_recv()
            j = s_m2 - m_begin
            at = pl.multiple_of(m_base + j * gm, 8)
            var_acc[pl.ds(at, gm), :] = square(got_mn[j] + part[s_m2, 3 * gm :] + got_mx[j])

        means(it)
        return carry

    def settle_y():
        for kind in table:
            def done(s, carry):
                kind.copy_y(s).wait_send()
                return carry

            lax.fori_loop(kind.begin, kind.begin + kind.number, done, 0)

        for s in range(m_begin, m_begin + m_number):
            for copy in m_y(s):
                copy.wait_send()

    def collect(is_end):
        for k in range(1, LINE):
            mean_copy(k).wait()
        total = mean_box[0]
        for index in range(1, LINE):
            total = total + mean_box[index]
        out_ref[: rows // 128, :] = total
        settle_y()
        for kind in table:
            def done(s, carry):
                if is_end:
                    for copy in (kind.first_b(s), kind.first_a(s), kind.swap(s)):
                        copy.wait_send()
                else:
                    for copy in (kind.cross_b(s), kind.back_b(s), kind.cross_a(s), kind.back_a(s)):
                        copy.wait_send()
                return carry

            lax.fori_loop(kind.begin, kind.begin + kind.number, done, 0)
        for s in range(m_begin, m_begin + m_number):
            for copy in m_first(s) if is_end else (m_cross(s),):
                copy.wait_send()
        for who in range(4):
            if is_end:
                mid_copy(1, who).wait_recv()
                pl.when(owner != who)(lambda: var_copy(1, who).wait_recv())
            else:
                var_copy(1, who).wait_recv()
                pl.when(owner != who)(lambda: mid_copy(1, who).wait_recv())
        for who in range(4):
            begin = rows // 128 + who * lines
            out_ref[begin : begin + lines - 1, :] = 1.0 - var_box[who, : lines - 1]
            out_ref[begin + lines - 1 : begin + lines, :] = 1.0 - (var_box[who, lines - 1 :] + mid_box[who])
        for k in range(1, count):
            (var_copy if is_end else mid_copy)(k, owner).wait_send()

    compute(0, True)
    pl.semaphore_wait(barrier, count - 1)
    total_turns = steps + max(LAG_X, LAG_A[3], LAG_M[2])

    @pl.when(ends)
    def _():
        lax.fori_loop(0, total_turns, end_turn, 0)
        for index in range(lines):
            var_box[owner, index : index + 1, :] = line_of(index)
        for k in range(1, count):
            var_copy(k, owner).start()
        collect(True)

    @pl.when(jnp.logical_not(ends))
    def _():
        lax.fori_loop(0, total_turns, middle_turn, 0)
        mid_box[owner] = line_of(lines - 1)
        for k in range(1, count):
            mid_copy(k, owner).start()
        collect(False)


def fused(test_points, train_points, weights, factor, *, count):
    dim, rows = test_points.shape
    local = train_points.shape[1]
    width = factor.shape[1]
    depth = -(-(dim + 16) // 128) * 128
    steps = rows // BLOCK
    dma = pltpu.SemaphoreType.DMA
    f32 = jnp.float32
    kinds, (_, m_number, gm, _) = kinds_of(rows)
    sems = [dma((steps,))] * 12 + [dma((m_number,))] * 8
    sems += [dma((LINE,)), dma((LINE,)), dma((count,)), dma((4,)), dma((4,))]
    boxes = [pltpu.VMEM((m_number, gm, width), f32)] * 5
    for _, number, gb, ga, _ in kinds:
        for size in (2 * ga, 2 * gb, 2 * gb, ga, ga, gb):
            boxes.append(pltpu.VMEM((number, size, width), f32))
    out = pl.pallas_call(
        functools.partial(kernel, count=count),
        out_shape=pltpu.VMEM((rows // 64, 128), f32),
        in_specs=[pl.BlockSpec(memory_space=pl.ANY)] * 4,
        out_specs=pl.BlockSpec(memory_space=pltpu.VMEM),
        scratch_shapes=[
            pltpu.VMEM((dim, rows), jnp.bfloat16),
            pltpu.VMEM((local // 128, 128), jnp.bfloat16),
            pltpu.VMEM((local, width), jnp.bfloat16),
            dma((3 + local // CHUNK,)),
            pltpu.VMEM((rows, depth), f32),
            pltpu.VMEM((depth, local), jnp.bfloat16),
            pltpu.VMEM((1, local), f32),
            pltpu.VMEM((BLOCK, depth), jnp.bfloat16),
            pltpu.VMEM((steps, BLOCK, width), f32),
            pltpu.VMEM((rows, 128), f32),
            pltpu.VMEM((rows // 4, 128), f32),
            pltpu.VMEM((LINE + 1, rows // 128, 128), f32),
            pltpu.VMEM((4, rows // 512, 128), f32),
            pltpu.VMEM((4, 1, 128), f32),
        ] + sems + boxes,
        compiler_params=pltpu.CompilerParams(
            collective_id=0, has_side_effects=True, vmem_limit_bytes=40 * 1024 * 1024
        ),
    )(*[pltpu.with_memory_space_constraint(x, pltpu.HBM) for x in (test_points, train_points, weights.reshape(local // 128, 128), factor)])
    lines = rows // 128
    return out[:lines].reshape(rows), out[lines:].reshape(rows)


def on_device(test_points, train_points, weights, factor):
    rows = test_points.shape[1]
    local = train_points.shape[1]
    dim = test_points.shape[0]
    width = factor.shape[1]
    test_sq = jnp.sum(test_points.astype(jnp.float32) ** 2, axis=0)
    block = math.gcd(local, 1024)
    turns = local // block

    def step(index, carry):
        mean_acc, proj_acc = carry
        start = (index * block).astype(jnp.int32)
        points = lax.dynamic_slice_in_dim(train_points, start, block, 1)
        wblock = lax.dynamic_slice_in_dim(weights, start, block, 0)
        fblock = lax.dynamic_slice_in_dim(factor, start, block, 0)
        train_sq = jnp.sum(points.astype(jnp.float32) ** 2, axis=0)
        cross = lax.dot_general(
            test_points, points, (((0,), (0,)), ((), ())), preferred_element_type=jnp.float32
        )
        kernel = jnp.exp(
            -(test_sq[:, None] + train_sq[None, :] - 2.0 * cross) * (4.0 / dim)
        ).astype(jnp.bfloat16)
        mean_acc = mean_acc + jnp.dot(kernel, wblock, preferred_element_type=jnp.float32)
        proj_acc = proj_acc + jnp.dot(kernel, fblock, preferred_element_type=jnp.float32)
        return (mean_acc, proj_acc)

    init = (jnp.zeros((rows,), jnp.float32), jnp.zeros((rows, width), jnp.float32))
    mean_part, proj_part = lax.fori_loop(0, turns, step, init)
    mean_share, proj_share = (
        lax.psum_scatter(mean_part, "trn", scatter_dimension=0, tiled=True),
        lax.psum_scatter(proj_part, "trn", scatter_dimension=0, tiled=True),
    )
    var_share = 1.0 - jnp.sum(proj_share * proj_share, axis=1)
    mean, variance = (
        lax.all_gather(mean_share, "trn", axis=0, tiled=True),
        lax.all_gather(var_share, "trn", axis=0, tiled=True),
    )
    return (mean, variance)


def solution(mesh):
    in_specs = (
        P(None, ("grp", "tst")),
        P(None, ("grp", "trn")),
        P(("grp", "trn")),
        P(("grp", "trn"), None),
    )
    out_specs = (P(("grp", "tst")), P(("grp", "tst")))
    count = mesh.shape["trn"]
    body = functools.partial(fused, count=count) if count == 2 * LINE else on_device
    return jax.shard_map(
        body, mesh=mesh, in_specs=in_specs, out_specs=out_specs, check_vma=False
    )
```
